128 devices in a mesh: ctx: 16 (over x, z), tp: 8 (over y, core).
Axes of the slice: x: 4, y: 4, z: 4, core: 2. Of those that a mesh axis runs over, the one named last changes fastest.
Arguments:
- queries: bfloat16 [512, 8192], P('ctx', 'tp'), may hold values from -6 to 6
- cache_keys: bfloat16 [65536, 1024], P('ctx', 'tp'), may hold values from -18 to 18
- cache_values: bfloat16 [65536, 1024], P('ctx', 'tp'), may hold values from -6 to 6
- span_keys: bfloat16 [512, 1024], P('ctx', 'tp'), may hold values from -24 to 24
- span_values: bfloat16 [512, 1024], P('ctx', 'tp'), may hold values from -6 to 6
- out_weight: bfloat16 [8192, 8192], P('tp', 'ctx'), may hold values from -0.0625 to 0.0625
- residual: bfloat16 [512, 8192], P('tp', 'ctx'), may hold values from -72 to 72
- norm_gain: bfloat16 [8192], P('ctx'), may hold values from 0.5 to 1.5
- head_weight: bfloat16 [8192, 128256], P(None, ('ctx', 'tp')), may hold values from -0.198873782 to 0.198873782
- targets: int32 [512], replicated, may hold values from 0 to 128255
- window_lengths: int32 [8], replicated, may hold values from 1 to 128, 512 in all
Outputs:
- token_logprob: float32 [512], P('ctx')
- window_means: float32 [8], replicated
The draws below stay inside these ranges and needn't reach their ends.
Inputs may be any that keep to these rules, and one draw needn't show every extreme that they name: `window_lengths`: the 8 lengths sum to 512.
All inputs are finite; a program needn't handle non-finite values.
Results may differ from the reference program's by a relative error of at most 0.0025.
Values may be sent and summed in bfloat16 or wider, within the bound.
No kernel may reach another device: no remote copies, remote signals or barrier semaphores. Data moves between devices by JAX's collectives and lax.ppermute only.
A program may use at most 128 MiB of HBM per device.

```python
import math
import jax
import jax.numpy as jnp
import numpy as np
from jax import lax

D = 8192
HEADS = 64
KV_HEADS = 8
HD = 128
VOCAB = 128256
WINDOW = 128
SPAN = 512
PREFIX = 65536
WINDOWS = 8


def draw_cache_keys(key, part):
    drawn = 3.0 * jnp.clip(jax.random.normal(jax.random.fold_in(key, 11), (PREFIX, KV_HEADS * HD), jnp.float32), -6.0, 6.0)
    return drawn.astype(jnp.bfloat16)


def draw_queries(key, part):
    drawn = jnp.clip(jax.random.normal(jax.random.fold_in(key, 12), (SPAN, HEADS * HD), jnp.float32), -6.0, 6.0)
    return drawn.astype(jnp.bfloat16)


def draw_head_weight(key, part):
    scaling = 3.0 * D ** (-0.5)
    drawn = scaling * jnp.clip(jax.random.normal(jax.random.fold_in(key, 13), (D, VOCAB), jnp.float32), -6.0, 6.0)
    return drawn.astype(jnp.bfloat16)


def draw_residual(key, part):
    column_scale = 0.6 + 1.2 * jnp.arange(D, dtype=jnp.float32) / (D - 1)
    drawn = jnp.clip(jax.random.normal(jax.random.fold_in(key, 14), (SPAN, D), jnp.float32), -4.0, 4.0) * column_scale[None, :]
    return drawn.astype(jnp.bfloat16)


def place_ends(drawn, stream_key, low, largest):
    index_at = [jax.random.randint(jax.random.fold_in(stream_key, axis), (), 0, length) for axis, length in enumerate(drawn.shape)]
    longest = drawn.shape.index(max(drawn.shape))
    neighbour = index_at[:longest] + [(index_at[longest] + 1) % drawn.shape[longest]] + index_at[longest + 1:]
    return drawn.at[tuple(index_at)].set(low).at[tuple(neighbour)].set(largest)


def level_of(key, dims, cuts, smallest, largest):
    level = 1.0
    for axis_at, shards_of in cuts:
        steps = jax.random.uniform(jax.random.fold_in(jax.random.fold_in(key, 6), axis_at), (shards_of,), jnp.float32, smallest / len(cuts), largest / len(cuts))
        level = level * jnp.repeat(jnp.exp(steps), dims[axis_at] // shards_of).reshape((-1,) + (1,) * (len(dims) - 1 - axis_at))
    return level


def wide_ids(key, dims, number_of, lean):
    portions = [min(1 << octave, number_of + 1 - (1 << octave)) * (1 << 20) // math.isqrt((1 << octave) ** lean) + 1 for octave in range((number_of + 1).bit_length()) if 1 << octave <= number_of]
    width = 1 + sum(portions) // (1 << 30)
    table = np.cumsum(np.array([max(1, weight // width) for weight in portions]))
    pick = jax.random.randint(jax.random.fold_in(key, 1), dims, 0, int(table[len(portions) - 1]))
    start = jnp.left_shift(1, jnp.searchsorted(jnp.asarray(table, jnp.int32), pick, side="right").astype(jnp.int32))
    standing = start - 1 + jax.random.randint(jax.random.fold_in(key, 4), dims, 0, 1 << 30) % jnp.minimum(start, number_of + 1 - start)
    return jax.random.permutation(jax.random.fold_in(key, 2), number_of)[standing].astype(jnp.int32)


def length_profile(count, total, limit, skew):
    portions = [(1 << 20) // math.isqrt(standing ** skew) + 1 for standing in range(2, count + 1)]
    spare, counts = total - limit - (count - 1), [1] * (count - 1)
    while spare > 0:
        movable = [i for i in range(count - 1) if counts[i] < limit]
        mass, budget = sum([portions[i] for i in movable]), spare
        for i in movable:
            more = min(limit - counts[i], max(1, budget * portions[i] // mass), spare)
            counts[i] = counts[i] + more
            spare = spare - more
    return np.array([limit] + counts)


def ragged_sizes(key, count, total, limit, slope):
    if count == 2:
        one = jax.random.randint(key, (), max(1, total - limit), min(limit, total - 1) + 1)
        return jnp.stack([one, total - one])
    tallies = jnp.asarray(length_profile(count, total, limit, slope), jnp.int32)
    couples = (count - 1) // 2
    source_of, receiver = tallies[1:1 + 2 * couples:2], tallies[2:2 + 2 * couples:2]
    room = jnp.minimum(source_of - 1, limit - receiver)
    shifted = jax.random.randint(jax.random.fold_in(key, 1), (couples,), 0, 1 << 20) % (room + 1)
    tallies = tallies.at[1:1 + 2 * couples:2].set(source_of - shifted).at[2:2 + 2 * couples:2].set(receiver + shifted)
    return tallies[jax.random.permutation(jax.random.fold_in(key, 2), count)]


def noise(rng, extent, scale, bound, split=(), held_as=jnp.bfloat16):
    level = level_of(rng, extent, split, -0.22, 0.18) if split else 1.0
    entries = jax.random.normal(rng, extent, jnp.float32) * scale * level
    return jnp.minimum(jnp.maximum(entries, -bound), bound).astype(held_as)


def setup_inputs(seed: int = 0) -> dict:
    streams_of = jax.random.split(jax.random.key(seed), 12)
    queries = draw_queries(jax.random.fold_in(streams_of[11], 71), 0)
    cache_keys = draw_cache_keys(jax.random.fold_in(streams_of[11], 71), 0)
    cache_values = noise(streams_of[2], (PREFIX, KV_HEADS * HD), 1.0, 6.0, ((0, 16), (1, 8)))
    span_keys = noise(streams_of[3], (SPAN, KV_HEADS * HD), 4.0, 24.0, ((0, 16), (1, 8)))
    span_values = noise(streams_of[4], (SPAN, KV_HEADS * HD), 1.0, 6.0, ((0, 16), (1, 8)))
    out_weight = noise(streams_of[5], (HEADS * HD, D), (HEADS * HD) ** -0.5, 0.0625, ((0, 8), (1, 16)))
    residual = draw_residual(jax.random.fold_in(streams_of[11], 71), 0)
    norm_gain = jnp.clip(1.0 + 0.1 * jax.random.normal(streams_of[7], (D,), jnp.float32), 0.5, 1.5).astype(jnp.bfloat16)
    head_weight = draw_head_weight(jax.random.fold_in(streams_of[11], 71), 0)
    targets = place_ends(wide_ids(streams_of[9], (SPAN,), VOCAB, 2), jax.random.fold_in(streams_of[9], 3), 0, VOCAB - 1).astype(jnp.int32)
    window_lengths = ragged_sizes(streams_of[10], WINDOWS, SPAN, WINDOW, 1).astype(jnp.int32)
    return {"queries": queries, "cache_keys": cache_keys, "cache_values": cache_values, "span_keys": span_keys, "span_values": span_values, "out_weight": out_weight, "residual": residual, "norm_gain": norm_gain, "head_weight": head_weight, "targets": targets, "window_lengths": window_lengths}


EPSILON = 1e-05
NEGATIVE = -1e+30

def fold_block(state, scores, value_rows):
    row_max, row_sum, weighted = state
    new_max = jnp.maximum(row_max, lax.optimization_barrier(jnp.max(scores, axis=1)))
    fading = jnp.exp(row_max - new_max)
    weights = jnp.exp(scores - new_max[:, None])
    row_sum = row_sum * fading + lax.optimization_barrier(jnp.sum(weights, axis=1))
    weighted = weighted * fading[:, None] + jnp.dot(weights.astype(jnp.bfloat16), value_rows, preferred_element_type=jnp.float32)
    return (new_max, row_sum, weighted)

def attend_head(bundle):
    query_rows, cache_part, value_part, fresh_keys, fresh_values = bundle
    row_count = query_rows.shape[0]
    scaling = HD ** (-0.5)
    block_size = min(1024, cache_part.shape[0])
    block_count = cache_part.shape[0] // block_size
    key_blocks = cache_part.reshape(block_count, block_size, HD)
    value_blocks = value_part.reshape(block_count, block_size, HD)

    def advance(state, block_pair):
        scores = jnp.dot(query_rows, block_pair[0].T, preferred_element_type=jnp.float32) * scaling
        return (fold_block(state, scores, block_pair[1]), None)
    start_state = (jnp.full((row_count,), NEGATIVE, jnp.float32), jnp.zeros((row_count,), jnp.float32), jnp.zeros((row_count, HD), jnp.float32))
    state, unused = lax.scan(advance, start_state, (key_blocks, value_blocks))
    scores = jnp.dot(query_rows, fresh_keys.T, preferred_element_type=jnp.float32) * scaling
    token_of_row = jnp.arange(row_count, dtype=jnp.int32) % SPAN
    key_token = jnp.arange(fresh_keys.shape[0], dtype=jnp.int32)
    scores = jnp.where(token_of_row[:, None] >= key_token[None, :], scores, NEGATIVE)
    row_max, row_sum, weighted = fold_block(state, scores, fresh_values)
    return (weighted / row_sum[:, None]).astype(jnp.bfloat16)

def reference(queries, cache_keys, cache_values, span_keys, span_values, out_weight, residual, norm_gain, head_weight, targets, window_lengths):
    group_size = HEADS // KV_HEADS
    query_heads = queries.reshape(SPAN, KV_HEADS, group_size, HD).transpose(1, 2, 0, 3).reshape(KV_HEADS, group_size * SPAN, HD)
    key_heads = cache_keys.reshape(PREFIX, KV_HEADS, HD).transpose(1, 0, 2)
    value_heads = cache_values.reshape(PREFIX, KV_HEADS, HD).transpose(1, 0, 2)
    fresh_key_heads = span_keys.reshape(SPAN, KV_HEADS, HD).transpose(1, 0, 2)
    fresh_value_heads = span_values.reshape(SPAN, KV_HEADS, HD).transpose(1, 0, 2)
    attended = lax.map(attend_head, (query_heads, key_heads, value_heads, fresh_key_heads, fresh_value_heads))
    attended = attended.reshape(KV_HEADS, group_size, SPAN, HD).transpose(2, 0, 1, 3).reshape(SPAN, HEADS * HD)
    stream = residual.astype(jnp.float32) + jnp.dot(attended, out_weight, preferred_element_type=jnp.float32)
    mean_square = lax.optimization_barrier(jnp.mean(stream * stream, axis=1))
    normed = (stream * lax.rsqrt(mean_square + EPSILON)[:, None] * norm_gain.astype(jnp.float32)[None, :]).astype(jnp.bfloat16)
    logits = jnp.dot(normed, head_weight, preferred_element_type=jnp.float32)
    row_max = lax.optimization_barrier(jnp.max(logits, axis=1))
    log_total = row_max + jnp.log(lax.optimization_barrier(jnp.sum(jnp.exp(logits - row_max[:, None]), axis=1)))
    target_logit = jnp.take_along_axis(logits, targets[:, None].astype(jnp.int32), axis=1)[:, 0]
    token_logprob = target_logit - log_total
    window_ends = jnp.cumsum(window_lengths).astype(jnp.int32)
    window_starts = window_ends - window_lengths
    positions = jnp.arange(SPAN, dtype=jnp.int32)
    member = ((positions[None, :] >= window_starts[:, None]) & (positions[None, :] < window_ends[:, None])).astype(jnp.float32)
    window_sums = jnp.dot(member, token_logprob, precision=lax.Precision.HIGHEST)
    window_means = window_sums / window_lengths.astype(jnp.float32)
    return (token_logprob, window_means)
```

```python
import jax
import jax.numpy as jnp
from jax import lax
from jax.experimental import pallas as pl
from jax.experimental.pallas import tpu as pltpu
from jax.sharding import Mesh
from jax.sharding import PartitionSpec as P

D = 8192
HEADS = 64
KV_HEADS = 8
HD = 128
GROUP = HEADS // KV_HEADS
CTX = ("ctx_0", "ctx_1")
TP = ("tp_0", "tp_1")
CTX_TP = ("ctx_0", "ctx_1", "tp_0", "tp_1")
EPSILON = 1e-05
NEGATIVE = -1e30
LOG2E = 1.4426950408889634
TO_LOG2 = HD ** (-0.5) * LOG2E
ROWS = 256
KEYS = 2048


def sent_to_all(value, axis):
    count = lax.axis_size(axis)
    return lax.all_to_all(
        jnp.broadcast_to(value[None], (count, *value.shape)), axis, 0, 0, tiled=True
    )


def whole(*shape):
    return pl.BlockSpec(shape, lambda *at: (0,) * len(shape))


def attend(first_token, queries, keys, values, fresh_keys, fresh_values, side):
    sources, span_dev, width = queries.shape
    span, cached, fresh = sources * span_dev, keys.shape[0], fresh_keys.shape[0]
    heads = width // HD
    total = cached + 128
    chunks = [(a, KEYS) for a in range(0, cached, KEYS)]
    chunks[-1] = (chunks[-1][0], total - chunks[-1][0])

    def body(first_ref, q_ref, k_ref, v_ref, fk_ref, fv_ref, side_ref, out_ref, kt, va, sbuf, mbuf):
        i = pl.program_id(0)

        @pl.when(i == 0)
        def _():
            for a in range(0, cached, 512):
                kt[:, a : a + 512] = k_ref[a : a + 512, :].T
            gap = jnp.zeros((128 - fresh, HD), jnp.bfloat16)
            kt[:, cached:] = jnp.concatenate([fk_ref[...], gap], 0).T
            va[:cached, :HD] = v_ref[...]
            va[cached:, :HD] = jnp.concatenate([fv_ref[...], gap], 0)
            va[:, HD:] = jnp.ones((total, HD), jnp.bfloat16)
            out_ref[:, :, width:] = jnp.broadcast_to(side_ref[...], (sources, span_dev, HD))

        def step(scoring, weighing):
            to = lax.rem(i, 2)
            at = lax.rem(i + 1, 2)
            for r in range(0, span, ROWS):
                rows = slice(r, r + ROWS)
                tokens = slice(r // span_dev, (r + ROWS) // span_dev)
                top, acc = None, None
                if scoring:
                    q = q_ref[tokens].reshape(ROWS, HD)
                if weighing:
                    shift = mbuf[at, rows, :]
                for a, n in chunks:
                    if scoring:
                        s = jnp.dot(q, kt[:, a : a + n], preferred_element_type=jnp.float32)
                        if a + n == total:
                            col = lax.broadcasted_iota(jnp.int32, (ROWS, 128), 1)
                            row = lax.broadcasted_iota(jnp.int32, (ROWS, 128), 0) + r
                            seen = (col < fresh) & (row >= col + first_ref[0])
                            tail = jnp.where(seen, s[:, n - 128 :], NEGATIVE)
                            s = jnp.concatenate([s[:, : n - 128], tail], 1)
                        sbuf[to, rows, a : a + n] = s
                        for b in range(0, n, 128):
                            piece = s[:, b : b + 128]
                            top = piece if top is None else jnp.maximum(top, piece)
                    if weighing:
                        p = jnp.concatenate(
                            [
                                jnp.exp2(
                                    sbuf[at, rows, a + b : a + b + 128] * TO_LOG2 - shift
                                ).astype(jnp.bfloat16)
                                for b in range(0, n, 128)
                            ],
                            1,
                        )
                        d = jnp.dot(p, va[a : a + n, :], preferred_element_type=jnp.float32)
                        acc = d if acc is None else acc + d
                if scoring:
                    m = jnp.max(top, axis=1, keepdims=True) * TO_LOG2
                    mbuf[to, rows, :] = jnp.broadcast_to(m, (ROWS, 128))
                if weighing:
                    h = i - 1
                    row_sum = acc[:, HD:]
                    o = (acc[:, :HD] / row_sum).astype(jnp.bfloat16)
                    place = pl.ds(pl.multiple_of(h * HD, HD), HD)
                    out_ref[tokens, :, place] = o.reshape(-1, span_dev, HD)
                    level = shift + jnp.log2(row_sum)
                    high = level.astype(jnp.bfloat16).astype(jnp.float32)
                    low = level - high
                    lane = lax.broadcasted_iota(jnp.int32, (ROWS, HD), 1)
                    old = out_ref[tokens, :, width:].reshape(ROWS, HD).astype(jnp.float32)
                    new = jnp.where(lane == h, high, jnp.where(lane == h + heads, low, old))
                    out_ref[tokens, :, width:] = new.astype(jnp.bfloat16).reshape(-1, span_dev, HD)

        @pl.when(i == 0)
        def _():
            step(True, False)

        @pl.when((i > 0) & (i < heads))
        def _():
            step(True, True)

        @pl.when(i == heads)
        def _():
            step(False, True)

    out_shape = (sources, span_dev, width + HD)
    return pl.pallas_call(
        body,
        out_shape=jax.ShapeDtypeStruct(out_shape, jnp.bfloat16),
        grid_spec=pltpu.PrefetchScalarGridSpec(
            num_scalar_prefetch=1,
            grid=(heads + 1,),
            in_specs=[
                pl.BlockSpec(
                    (sources, span_dev, HD), lambda i, f: (0, 0, jnp.minimum(i, heads - 1))
                ),
                whole(cached, HD),
                whole(cached, HD),
                whole(fresh, HD),
                whole(fresh, HD),
                whole(1, span_dev, HD),
            ],
            out_specs=whole(*out_shape),
            scratch_shapes=[
                pltpu.VMEM((HD, total), jnp.bfloat16),
                pltpu.VMEM((total, 2 * HD), jnp.bfloat16),
                pltpu.VMEM((2, span, total), jnp.float32),
                pltpu.VMEM((2, span, HD), jnp.float32),
            ],
        ),
        compiler_params=pltpu.CompilerParams(
            dimension_semantics=("arbitrary",), vmem_limit_bytes=48 << 20
        ),
        cost_estimate=pl.CostEstimate(
            flops=4 * heads * span * total * HD,
            transcendentals=heads * span * total,
            bytes_accessed=6 << 20,
        ),
        name="attend",
    )(first_token, queries, keys, values, fresh_keys, fresh_values, side)


def merge(pieces, copies):
    sources, span_dev, wide = pieces.shape
    width = wide - HD
    heads = width // HD

    def body(in_ref, out_ref):
        tail = in_ref[:, :, width:].astype(jnp.float32).reshape(sources * span_dev, HD)
        level = (tail + pltpu.roll(tail, HD - heads, 1)).reshape(sources, span_dev, HD)
        top = jnp.max(level, axis=0)
        weight = jnp.exp2(level - top[None])
        weight = weight / jnp.sum(weight, axis=0)[None]
        for h in range(heads):
            cols = slice(h * HD, (h + 1) * HD)
            acc = None
            for k in range(sources):
                part = in_ref[k, :, cols].astype(jnp.float32) * weight[k][:, h : h + 1]
                acc = part if acc is None else acc + part
            acc = acc.astype(jnp.bfloat16)
            for k in range(copies):
                out_ref[k, :, cols] = acc

    return pl.pallas_call(
        body,
        out_shape=jax.ShapeDtypeStruct((copies, span_dev, width), jnp.bfloat16),
        in_specs=[whole(*pieces.shape)],
        out_specs=whole(copies, span_dev, width),
        grid=(1,),
        name="merge",
    )(pieces)


def score(rows, inverse, weight, local_target):
    tps, parts, tokens, cols = rows.shape
    span = tps * tokens
    vocab = weight.shape[1]
    per = 2
    steps = parts // per

    def body(x_ref, inv_ref, w_ref, t_ref, out_ref, acc, squares):
        i = pl.program_id(0)
        total, ss = None, None
        for k in range(per):
            x = x_ref[:, k].reshape(span, cols)
            d = jnp.dot(x, w_ref[k * cols : (k + 1) * cols, :], preferred_element_type=jnp.float32)
            total = d if total is None else total + d
            xf = x.astype(jnp.float32)
            sq = xf * xf * inv_ref[k]
            for b in range(0, cols, 128):
                piece = sq[:, b : b + 128]
                ss = piece if ss is None else ss + piece

        @pl.when(i == 0)
        def _():
            acc[...] = total
            squares[...] = ss

        @pl.when(i > 0)
        def _():
            acc[...] += total
            squares[...] += ss

        @pl.when(i == steps - 1)
        def _():
            mean = jnp.sum(squares[...], axis=1, keepdims=True) / D
            logits = acc[...] * lax.rsqrt(mean + EPSILON)
            col = lax.broadcasted_iota(jnp.int32, (span, vocab), 1)
            top = jnp.max(logits, axis=1, keepdims=True)
            sums = jnp.sum(jnp.exp(logits - top), axis=1, keepdims=True)
            level = top + jnp.log(sums)
            hit = jnp.sum(jnp.where(col == t_ref[...], logits, 0.0), axis=1, keepdims=True)
            lane = lax.broadcasted_iota(jnp.int32, (span, 128), 1)
            both = jnp.where(lane == 0, level, hit)
            out_ref[...] = both.T[:2, :]

    return pl.pallas_call(
        body,
        out_shape=jax.ShapeDtypeStruct((2, span), jnp.float32),
        grid=(steps,),
        in_specs=[
            pl.BlockSpec((tps, per, tokens, cols), lambda i: (0, i, 0, 0)),
            pl.BlockSpec((per, 1, cols), lambda i: (i, 0, 0)),
            pl.BlockSpec((per * cols, vocab), lambda i: (i, 0)),
            whole(span, 1),
        ],
        out_specs=whole(2, span),
        scratch_shapes=[
            pltpu.VMEM((span, vocab), jnp.float32),
            pltpu.VMEM((span, 128), jnp.float32),
        ],
        compiler_params=pltpu.CompilerParams(
            dimension_semantics=("arbitrary",), vmem_limit_bytes=48 << 20
        ),
        cost_estimate=pl.CostEstimate(
            flops=2 * span * D * vocab, transcendentals=span * vocab, bytes_accessed=26 << 20
        ),
        name="score",
    )(rows, inverse, weight, local_target)


def joined(level_hit, axis):
    pieces = sent_to_all(level_hit, axis)
    level, hit = pieces[:, 0], pieces[:, 1]
    top = jnp.max(level, axis=0)
    total = top + jnp.log(jnp.sum(jnp.exp(level - top[None]), axis=0))
    return jnp.stack([total, jnp.sum(hit, axis=0)])


def local(
    queries,
    cache_keys,
    cache_values,
    span_keys,
    span_values,
    out_weight,
    residual,
    norm_gain,
    head_weight,
    targets,
    window_lengths,
):
    ctx_rank = lax.axis_index(CTX)
    span_dev, width = queries.shape
    ctx_size, tp_size = lax.axis_size(CTX), lax.axis_size(TP)
    span_total = span_dev * ctx_size
    first_token = ctx_rank * span_dev
    model_dev = norm_gain.shape[0]
    gain_lanes = model_dev // span_dev
    side = jnp.pad(
        norm_gain.reshape(1, span_dev, gain_lanes),
        ((0, 0), (0, 0), (2 * GROUP, HD - 2 * GROUP - gain_lanes)),
    )
    partial = attend(
        first_token.reshape(1),
        sent_to_all(queries, CTX),
        cache_keys,
        cache_values,
        span_keys,
        span_values,
        side,
    )
    pieces = lax.all_to_all(partial, CTX, split_axis=0, concat_axis=0, tiled=True)
    gains = pieces[:, :, width + 2 * GROUP : width + 2 * GROUP + gain_lanes]
    gains = gains.reshape(ctx_size, 1, model_dev).astype(jnp.float32)
    inverse = 1.0 / (gains * gains)
    attended = lax.all_to_all(merge(pieces, ctx_size), CTX, split_axis=0, concat_axis=0, tiled=True)
    projected = jnp.dot(
        attended.reshape(span_total, width), out_weight, preferred_element_type=jnp.float32
    ).astype(jnp.bfloat16)
    arrived = lax.all_to_all(
        projected.reshape(tp_size, span_total // tp_size, model_dev), TP, 0, 0, tiled=True
    )
    stream = residual.astype(jnp.float32) + arrived.astype(jnp.float32).sum(axis=0)
    gained = (stream * norm_gain.astype(jnp.float32)[None, :]).astype(jnp.bfloat16)
    rows = lax.all_gather(sent_to_all(gained, CTX), TP)
    vocab_dev = head_weight.shape[1]
    local_target = (targets - lax.axis_index(CTX_TP) * vocab_dev).reshape(span_total, 1)
    level_hit = score(rows, inverse, head_weight, local_target)
    level_hit = joined(joined(level_hit, CTX), TP)
    token_logprob = level_hit[1] - level_hit[0]
    window_ends = jnp.cumsum(window_lengths)
    window_starts = window_ends - window_lengths
    positions = jnp.arange(span_total, dtype=jnp.int32)
    member = (positions[None, :] >= window_starts[:, None]) & (
        positions[None, :] < window_ends[:, None]
    )
    window_sums = jnp.sum(jnp.where(member, token_logprob[None, :], 0.0), axis=1)
    window_means = window_sums / window_lengths.astype(jnp.float32)
    own_logprob = lax.dynamic_slice_in_dim(token_logprob, first_token, span_dev, 0)
    return (own_logprob, window_means)


def solution(mesh):
    split = Mesh(mesh.devices.reshape(4, 4, 4, 2), ("ctx_0", "ctx_1", "tp_0", "tp_1"))
    in_specs = (
        P(CTX, TP),
        P(CTX, TP),
        P(CTX, TP),
        P(CTX, TP),
        P(CTX, TP),
        P(TP, CTX),
        P(TP, CTX),
        P(CTX),
        P(None, CTX_TP),
        P(),
        P(),
    )
    out_specs = (P(CTX), P())
    return jax.shard_map(local, mesh=split, in_specs=in_specs, out_specs=out_specs, check_vma=False)
```

```python
import jax
import jax.numpy as jnp
from jax import lax
from jax.experimental import pallas as pl
from jax.experimental.pallas import tpu as pltpu
from jax.sharding import Mesh
from jax.sharding import PartitionSpec as P

D = 8192
HEADS = 64
KV_HEADS = 8
HD = 128
GROUP = HEADS // KV_HEADS
CTX = ("ctx_0", "ctx_1")
TP = ("tp_0", "tp_1")
CTX_TP = ("ctx_0", "ctx_1", "tp_0", "tp_1")
EPSILON = 1e-05
NEGATIVE = -1e30
LOG2E = 1.4426950408889634
TO_LOG2 = HD ** (-0.5) * LOG2E
ROWS = 256
KEYS = 2048


def sent_to_all(value, axis):
    count = lax.axis_size(axis)
    return lax.all_to_all(
        jnp.broadcast_to(value[None], (count, *value.shape)), axis, 0, 0, tiled=True
    )


def whole(*shape):
    return pl.BlockSpec(shape, lambda *at: (0,) * len(shape))


def attend(first_token, queries, keys, values, fresh_keys, fresh_values, side):
    sources, span_dev, width = queries.shape
    span, cached, fresh = sources * span_dev, keys.shape[0], fresh_keys.shape[0]
    heads = width // HD
    total = cached + 128
    chunks = [(a, KEYS) for a in range(0, cached, KEYS)]
    chunks[-1] = (chunks[-1][0], total - chunks[-1][0])

    def body(first_ref, q_ref, k_ref, v_ref, fk_ref, fv_ref, side_ref, out_ref, kt, va, sbuf, mbuf):
        i = pl.program_id(0)

        @pl.when(i == 0)
        def _():
            for a in range(0, cached, 512):
                kt[:, a : a + 512] = k_ref[a : a + 512, :].T
            gap = jnp.zeros((128 - fresh, HD), jnp.bfloat16)
            kt[:, cached:] = jnp.concatenate([fk_ref[...], gap], 0).T
            va[:cached, :HD] = v_ref[...]
            va[cached:, :HD] = jnp.concatenate([fv_ref[...], gap], 0)
            va[:, HD:] = jnp.ones((total, HD), jnp.bfloat16)
            out_ref[:, :, width:] = jnp.broadcast_to(side_ref[...], (sources, span_dev, HD))

        def step(scoring, weighing):
            to = lax.rem(i, 2)
            at = lax.rem(i + 1, 2)
            for r in range(0, span, ROWS):
                rows = slice(r, r + ROWS)
                tokens = slice(r // span_dev, (r + ROWS) // span_dev)
                top, acc = None, None
                if scoring:
                    q = q_ref[tokens].reshape(ROWS, HD)
                if weighing:
                    shift = mbuf[at, rows, :]
                for a, n in chunks:
                    if scoring:
                        s = jnp.dot(q, kt[:, a : a + n], preferred_element_type=jnp.float32)
                        if a + n == total:
                            col = lax.broadcasted_iota(jnp.int32, (ROWS, 128), 1)
                            row = lax.broadcasted_iota(jnp.int32, (ROWS, 128), 0) + r
                            seen = (col < fresh) & (row >= col + first_ref[0])
                            tail = jnp.where(seen, s[:, n - 128 :], NEGATIVE)
                            s = jnp.concatenate([s[:, : n - 128], tail], 1)
                        sbuf[to, rows, a : a + n] = s
                        for b in range(0, n, 128):
                            piece = s[:, b : b + 128]
                            top = piece if top is None else jnp.maximum(top, piece)
                    if weighing:
                        p = jnp.concatenate(
                            [
                                jnp.exp2(
                                    sbuf[at, rows, a + b : a + b + 128] * TO_LOG2 - shift
                                ).astype(jnp.bfloat16)
                                for b in range(0, n, 128)
                            ],
                            1,
                        )
                        d = jnp.dot(p, va[a : a + n, :], preferred_element_type=jnp.float32)
                        acc = d if acc is None else acc + d
                if scoring:
                    m = jnp.max(top, axis=1, keepdims=True) * TO_LOG2
                    mbuf[to, rows, :] = jnp.broadcast_to(m, (ROWS, 128))
                if weighing:
                    h = i - 1
                    row_sum = acc[:, HD:]
                    o = (acc[:, :HD] / row_sum).astype(jnp.bfloat16)
                    place = pl.ds(pl.multiple_of(h * HD, HD), HD)
                    out_ref[tokens, :, place] = o.reshape(-1, span_dev, HD)
                    level = shift + jnp.log2(row_sum)
                    high = level.astype(jnp.bfloat16).astype(jnp.float32)
                    low = level - high
                    lane = lax.broadcasted_iota(jnp.int32, (ROWS, HD), 1)
                    old = out_ref[tokens, :, width:].reshape(ROWS, HD).astype(jnp.float32)
                    new = jnp.where(lane == h, high, jnp.where(lane == h + heads, low, old))
                    out_ref[tokens, :, width:] = new.astype(jnp.bfloat16).reshape(-1, span_dev, HD)

        @pl.when(i == 0)
        def _():
            step(True, False)

        @pl.when((i > 0) & (i < heads))
        def _():
            step(True, True)

        @pl.when(i == heads)
        def _():
            step(False, True)

    out_shape = (sources, span_dev, width + HD)
    return pl.pallas_call(
        body,
        out_shape=jax.ShapeDtypeStruct(out_shape, jnp.bfloat16),
        grid_spec=pltpu.PrefetchScalarGridSpec(
            num_scalar_prefetch=1,
            grid=(heads + 1,),
            in_specs=[
                pl.BlockSpec(
                    (sources, span_dev, HD), lambda i, f: (0, 0, jnp.minimum(i, heads - 1))
                ),
                whole(cached, HD),
                whole(cached, HD),
                whole(fresh, HD),
                whole(fresh, HD),
                whole(1, span_dev, HD),
            ],
            out_specs=whole(*out_shape),
            scratch_shapes=[
                pltpu.VMEM((HD, total), jnp.bfloat16),
                pltpu.VMEM((total, 2 * HD), jnp.bfloat16),
                pltpu.VMEM((2, span, total), jnp.float32),
                pltpu.VMEM((2, span, HD), jnp.float32),
            ],
        ),
        compiler_params=pltpu.CompilerParams(
            dimension_semantics=("arbitrary",), vmem_limit_bytes=48 << 20
        ),
        cost_estimate=pl.CostEstimate(
            flops=4 * heads * span * total * HD,
            transcendentals=heads * span * total,
            bytes_accessed=6 << 20,
        ),
        name="attend",
    )(first_token, queries, keys, values, fresh_keys, fresh_values, side)


def merge(pieces, copies):
    sources, span_dev, wide = pieces.shape
    width = wide - HD
    heads = width // HD

    def body(in_ref, out_ref):
        tail = in_ref[:, :, width:].astype(jnp.float32).reshape(sources * span_dev, HD)
        level = (tail + pltpu.roll(tail, HD - heads, 1)).reshape(sources, span_dev, HD)
        top = jnp.max(level, axis=0)
        weight = jnp.exp2(level - top[None])
        weight = weight / jnp.sum(weight, axis=0)[None]
        for h in range(heads):
            cols = slice(h * HD, (h + 1) * HD)
            acc = None
            for k in range(sources):
                part = in_ref[k, :, cols].astype(jnp.float32) * weight[k][:, h : h + 1]
                acc = part if acc is None else acc + part
            acc = acc.astype(jnp.bfloat16)
            for k in range(copies):
                out_ref[k, :, cols] = acc

    return pl.pallas_call(
        body,
        out_shape=jax.ShapeDtypeStruct((copies, span_dev, width), jnp.bfloat16),
        in_specs=[whole(*pieces.shape)],
        out_specs=whole(copies, span_dev, width),
        grid=(1,),
        name="merge",
    )(pieces)


def score(chunks, places, inverse, own, partner, state, local_target):
    blocks, span, cols = chunks[0].shape
    count = len(chunks)
    vocab = own.shape[0]
    first, last = state is None, local_target is not None
    across = (((1,), (1,)), ((), ()))

    def body(*refs):
        refs = list(refs[1:])
        take = lambda n: [refs.pop(0) for _ in range(n)]
        x_refs, inv_refs, own_refs, partner_refs = (take(count) for _ in range(4))
        old = [] if first else take(2)
        t_ref = take(1)[0] if last else None
        acc, squares = (refs[1], refs[2]) if last else (refs[0], refs[1])
        i = pl.program_id(0)

        @pl.when(i == 0)
        def _():
            acc[...] = jnp.zeros_like(acc) if first else old[0][...]
            squares[...] = jnp.zeros_like(squares) if first else old[1][...]

        ss = None
        for side, w_refs in enumerate((own_refs, partner_refs)):
            total = None
            for x_ref, w_ref in zip(x_refs, w_refs):
                d = lax.dot_general(
                    w_ref[...], x_ref[0], across, preferred_element_type=jnp.float32
                )
                total = d if total is None else total + d
            acc[side] += total
        for x_ref, inv_ref in zip(x_refs, inv_refs):
            xf = x_ref[0].astype(jnp.float32)
            sq = xf * xf * inv_ref[0]
            for b in range(0, cols, 128):
                piece = sq[:, b : b + 128]
                ss = piece if ss is None else ss + piece
        squares[...] += ss

        if last:

            @pl.when(i == blocks - 1)
            def _():
                mean = jnp.sum(squares[...].T, axis=0, keepdims=True) / D
                scale = lax.rsqrt(mean + EPSILON)
                row = lax.broadcasted_iota(jnp.int32, (vocab, span), 0)
                logits = [acc[side] * scale for side in range(2)]
                top = jnp.max(jnp.maximum(*logits), axis=0, keepdims=True)
                sums = sum(
                    jnp.sum(jnp.exp(part - top), axis=0, keepdims=True) for part in logits
                )
                hit = sum(
                    jnp.sum(
                        jnp.where(row == t_ref[side : side + 1, :], logits[side], 0.0),
                        axis=0,
                        keepdims=True,
                    )
                    for side in range(2)
                )
                refs[0][...] = jnp.concatenate([top + jnp.log(sums), hit], 0)

    kept = [(2, vocab, span), (span, 128)]
    kept_shape = tuple(jax.ShapeDtypeStruct(k, jnp.float32) for k in kept)
    pick = lambda n: pl.BlockSpec((1, 1, cols), lambda i, at: (at[n, i], 0, 0))
    weigh = lambda n: pl.BlockSpec((vocab, cols), lambda i, at: (0, at[n, i]))
    in_specs = [pl.BlockSpec((1, span, cols), lambda i, at: (i, 0, 0))] * count
    in_specs += [pick(n) for n in range(count)]
    in_specs += [weigh(n) for n in range(count)] * 2
    operands = [*chunks, *[inverse] * count, *[own] * count, *[partner] * count]
    if not first:
        in_specs += [whole(*k) for k in kept]
        operands += state
    if last:
        in_specs.append(whole(2, span))
        operands.append(local_target)
        out_shape, out_specs = jax.ShapeDtypeStruct((2, span), jnp.float32), whole(2, span)
        scratch = [pltpu.VMEM(k, jnp.float32) for k in kept]
    else:
        out_shape, out_specs, scratch = kept_shape, tuple(whole(*k) for k in kept), []
    return pl.pallas_call(
        body,
        out_shape=out_shape,
        grid_spec=pltpu.PrefetchScalarGridSpec(
            num_scalar_prefetch=1,
            grid=(blocks,),
            in_specs=in_specs,
            out_specs=out_specs,
            scratch_shapes=scratch,
        ),
        compiler_params=pltpu.CompilerParams(
            dimension_semantics=("arbitrary",), vmem_limit_bytes=40 << 20
        ),
        cost_estimate=pl.CostEstimate(
            flops=4 * span * blocks * count * cols * vocab,
            transcendentals=2 * span * vocab if last else 0,
            bytes_accessed=4 * blocks * count * cols * vocab,
        ),
        name="score",
    )(places, *operands)


def shifted(value, axis, by):
    count = lax.axis_size(axis)
    return lax.ppermute(value, axis, [(i, (i + by) % count) for i in range(count)])


def local(
    queries,
    cache_keys,
    cache_values,
    span_keys,
    span_values,
    out_weight,
    residual,
    norm_gain,
    head_weight,
    targets,
    window_lengths,
):
    x, z = lax.axis_index("ctx_0"), lax.axis_index("ctx_1")
    y, core = lax.axis_index("tp_0"), lax.axis_index("tp_1")
    xs, zs, ys = (lax.axis_size(name) for name in ("ctx_0", "ctx_1", "tp_0"))
    ctx_rank = lax.axis_index(CTX)
    span_dev, width = queries.shape
    ctx_size = lax.axis_size(CTX)
    span_total = span_dev * ctx_size
    first_token = ctx_rank * span_dev
    model_dev = norm_gain.shape[0]
    own_weight = head_weight.T
    partner_weight = shifted(own_weight, "tp_1", 1)
    gain_lanes = model_dev // span_dev
    side = jnp.pad(
        norm_gain.reshape(1, span_dev, gain_lanes),
        ((0, 0), (0, 0), (2 * GROUP, HD - 2 * GROUP - gain_lanes)),
    )
    partial = attend(
        first_token.reshape(1),
        sent_to_all(queries, CTX),
        cache_keys,
        cache_values,
        span_keys,
        span_values,
        side,
    )
    pieces = lax.all_to_all(partial, CTX, split_axis=0, concat_axis=0, tiled=True)
    half = model_dev // 2
    gains = pieces[:, :, width + 2 * GROUP : width + 2 * GROUP + gain_lanes]
    gains = gains.reshape(2 * ctx_size, 1, half).astype(jnp.float32)
    inverse = 1.0 / (gains * gains)
    attended = lax.all_to_all(merge(pieces, ctx_size), CTX, split_axis=0, concat_axis=0, tiled=True)

    tokens = span_total // (2 * ys)
    by_core = attended.reshape(ys, 2, tokens, width)

    def projected(which):
        rows = lax.dynamic_index_in_dim(by_core, which, 1, keepdims=False)
        return jnp.dot(
            rows.reshape(ys * tokens, width), out_weight, preferred_element_type=jnp.float32
        )

    arrived = shifted(projected(1 - core).astype(jnp.bfloat16), "tp_1", 1)
    both = projected(core) + arrived.astype(jnp.float32)
    both = both.reshape(ys, tokens, model_dev)
    stream = residual.astype(jnp.float32) + lax.dynamic_index_in_dim(both, y, 0, keepdims=False)
    sent = both.astype(jnp.bfloat16)
    for by in range(1, ys):
        block = lax.dynamic_index_in_dim(sent, (y + by) % ys, 0, keepdims=False)
        stream = stream + shifted(block, "tp_0", by).astype(jnp.float32)
    gained = (stream * norm_gain.astype(jnp.float32)[None, :]).astype(jnp.bfloat16)
    rows = [gained] + [shifted(gained, "tp_0", by) for by in range(1, ys)]
    rows = jnp.concatenate(rows, 0)

    def places(steps, part):
        dx = jnp.array([s[0] for s in steps], jnp.int32)
        dz = jnp.array([s[1] for s in steps], jnp.int32)
        return 2 * (((x + dx) % xs) * zs + (z + dz) % zs) + part

    def gathered(value, first, second):
        behind, ahead = shifted(value, first, 1), shifted(value, first, -1)
        across = shifted(behind, first, 1)
        near = jnp.stack([value, behind, ahead, across])
        left, right = shifted(near, second, 1), shifted(near, second, -1)
        far = (shifted(left[:2], second, 1), shifted(right[2:], second, -1))
        return near, (left, right), far

    order = (0, -1, 1, -2)
    near_a, next_a, far_a = gathered(rows[:, :half], "ctx_1", "ctx_0")
    near_b, next_b, far_b = gathered(rows[:, half:], "ctx_0", "ctx_1")
    at_a = lambda step, among: places([(step, o) for o in among], 0)
    at_b = lambda step, among: places([(o, step) for o in among], 1)
    vocab_dev = head_weight.shape[1]
    mine = lax.dynamic_index_in_dim(targets.reshape(ys, 2, tokens), core, 1, keepdims=False)
    turn = (y - jnp.arange(ys, dtype=jnp.int32)) % ys
    turned = turn[:, None] == jnp.arange(ys, dtype=jnp.int32)[None, :]
    mine = jnp.sum(jnp.where(turned[:, :, None], mine[None], 0), axis=1).reshape(1, -1)
    rank = lax.axis_index(CTX_TP)
    starts = jnp.stack([rank, rank + 1 - 2 * core]) * vocab_dev
    local_target = mine - starts[:, None]
    state = score(
        (near_a, near_b),
        jnp.stack([at_a(0, order), at_b(0, order)]),
        inverse,
        own_weight,
        partner_weight,
        None,
        None,
    )
    state = score(
        (*next_a, *next_b),
        jnp.stack([at_a(-1, order), at_a(1, order), at_b(-1, order), at_b(1, order)]),
        inverse,
        own_weight,
        partner_weight,
        state,
        None,
    )
    level_hit = score(
        (*far_a, *far_b),
        jnp.stack(
            [at_a(-2, order[:2]), at_a(-2, order[2:]), at_b(-2, order[:2]), at_b(-2, order[2:])]
        ),
        inverse,
        own_weight,
        partner_weight,
        state,
        local_target,
    )
    level_hit = level_hit.reshape(2, ys, 1, tokens)
    level_hit = jnp.sum(jnp.where(turned.T[None, :, :, None], level_hit.reshape(2, 1, ys, tokens), 0.0), axis=2)
    gathered_stats = sent_to_all(level_hit.reshape(2, ys * tokens), ("ctx_0", "ctx_1", "tp_0"))
    level, hit = gathered_stats[:, 0], gathered_stats[:, 1]
    top = jnp.max(level, axis=0)
    total = top + jnp.log(jnp.sum(jnp.exp(level - top[None]), axis=0))
    my_logprob = jnp.sum(hit, axis=0) - total
    other_logprob = shifted(my_logprob, "tp_1", 1)
    pair = jnp.stack([my_logprob.reshape(ys, tokens), other_logprob.reshape(ys, tokens)], 1)
    token_logprob = jnp.where(core == 0, pair, pair[:, ::-1]).reshape(span_total)
    window_ends = jnp.cumsum(window_lengths)
    window_starts = window_ends - window_lengths
    positions = jnp.arange(span_total, dtype=jnp.int32)
    member = (positions[None, :] >= window_starts[:, None]) & (
        positions[None, :] < window_ends[:, None]
    )
    window_sums = jnp.sum(jnp.where(member, token_logprob[None, :], 0.0), axis=1)
    window_means = window_sums / window_lengths.astype(jnp.float32)
    own_logprob = lax.dynamic_slice_in_dim(token_logprob, first_token, span_dev, 0)
    return (own_logprob, window_means)


def solution(mesh):
    split = Mesh(mesh.devices.reshape(4, 4, 4, 2), ("ctx_0", "ctx_1", "tp_0", "tp_1"))
    in_specs = (
        P(CTX, TP),
        P(CTX, TP),
        P(CTX, TP),
        P(CTX, TP),
        P(CTX, TP),
        P(TP, CTX),
        P(TP, CTX),
        P(CTX),
        P(None, CTX_TP),
        P(),
        P(),
    )
    out_specs = (P(CTX), P())
    return jax.shard_map(local, mesh=split, in_specs=in_specs, out_specs=out_specs, check_vma=False)
```

```python
import jax
import jax.numpy as jnp
from jax import lax
from jax.experimental import pallas as pl
from jax.experimental.pallas import tpu as pltpu
from jax.sharding import Mesh
from jax.sharding import PartitionSpec as P

D = 8192
HEADS = 64
KV_HEADS = 8
HD = 128
GROUP = HEADS // KV_HEADS
CTX = ("ctx_0", "ctx_1")
TP = ("tp_0", "tp_1")
CTX_TP = ("ctx_0", "ctx_1", "tp_0", "tp_1")
EPSILON = 1e-05
NEGATIVE = -1e30
LOG2E = 1.4426950408889634
TO_LOG2 = HD ** (-0.5) * LOG2E
ROWS = 256
KEYS = 2048


def sent_to_all(value, axis):
    count = lax.axis_size(axis)
    return lax.all_to_all(
        jnp.broadcast_to(value[None], (count, *value.shape)), axis, 0, 0, tiled=True
    )


def whole(*shape):
    return pl.BlockSpec(shape, lambda *at: (0,) * len(shape))


def attend(first_token, queries, keys, values, fresh_keys, fresh_values, side):
    sources, span_dev, width = queries.shape
    span, cached, fresh = sources * span_dev, keys.shape[0], fresh_keys.shape[0]
    heads = width // HD
    total = cached + 128
    chunks = [(a, KEYS) for a in range(0, cached, KEYS)]
    chunks[-1] = (chunks[-1][0], total - chunks[-1][0])

    def body(first_ref, q_ref, k_ref, v_ref, fk_ref, fv_ref, side_ref, out_ref, kt, va, sbuf, mbuf):
        i = pl.program_id(0)

        @pl.when(i == 0)
        def _():
            for a in range(0, cached, 512):
                kt[:, a : a + 512] = k_ref[a : a + 512, :].T
            gap = jnp.zeros((128 - fresh, HD), jnp.bfloat16)
            kt[:, cached:] = jnp.concatenate([fk_ref[...], gap], 0).T
            va[:cached, :HD] = v_ref[...]
            va[cached:, :HD] = jnp.concatenate([fv_ref[...], gap], 0)
            va[:, HD:] = jnp.ones((total, HD), jnp.bfloat16)
            out_ref[:, :, width:] = jnp.broadcast_to(side_ref[...], (sources, span_dev, HD))

        def step(scoring, weighing):
            to = lax.rem(i, 2)
            at = lax.rem(i + 1, 2)
            for r in range(0, span, ROWS):
                rows = slice(r, r + ROWS)
                tokens = slice(r // span_dev, (r + ROWS) // span_dev)
                top, acc = None, None
                if scoring:
                    q = q_ref[tokens].reshape(ROWS, HD)
                if weighing:
                    shift = mbuf[at, rows, :]
                for a, n in chunks:
                    if scoring:
                        s = jnp.dot(q, kt[:, a : a + n], preferred_element_type=jnp.float32)
                        if a + n == total:
                            col = lax.broadcasted_iota(jnp.int32, (ROWS, 128), 1)
                            row = lax.broadcasted_iota(jnp.int32, (ROWS, 128), 0) + r
                            seen = (col < fresh) & (row >= col + first_ref[0])
                            tail = jnp.where(seen, s[:, n - 128 :], NEGATIVE)
                            s = jnp.concatenate([s[:, : n - 128], tail], 1)
                        sbuf[to, rows, a : a + n] = s
                        for b in range(0, n, 128):
                            piece = s[:, b : b + 128]
                            top = piece if top is None else jnp.maximum(top, piece)
                    if weighing:
                        p = jnp.concatenate(
                            [
                                jnp.exp2(
                                    sbuf[at, rows, a + b : a + b + 128] * TO_LOG2 - shift
                                ).astype(jnp.bfloat16)
                                for b in range(0, n, 128)
                            ],
                            1,
                        )
                        d = jnp.dot(p, va[a : a + n, :], preferred_element_type=jnp.float32)
                        acc = d if acc is None else acc + d
                if scoring:
                    m = jnp.max(top, axis=1, keepdims=True) * TO_LOG2
                    mbuf[to, rows, :] = jnp.broadcast_to(m, (ROWS, 128))
                if weighing:
                    h = i - 1
                    row_sum = acc[:, HD:]
                    o = (acc[:, :HD] / row_sum).astype(jnp.bfloat16)
                    place = pl.ds(pl.multiple_of(h * HD, HD), HD)
                    out_ref[tokens, :, place] = o.reshape(-1, span_dev, HD)
                    level = shift + jnp.log2(row_sum)
                    high = level.astype(jnp.bfloat16).astype(jnp.float32)
                    low = level - high
                    lane = lax.broadcasted_iota(jnp.int32, (ROWS, HD), 1)
                    old = out_ref[tokens, :, width:].reshape(ROWS, HD).astype(jnp.float32)
                    new = jnp.where(lane == h, high, jnp.where(lane == h + heads, low, old))
                    out_ref[tokens, :, width:] = new.astype(jnp.bfloat16).reshape(-1, span_dev, HD)

        @pl.when(i == 0)
        def _():
            step(True, False)

        @pl.when((i > 0) & (i < heads))
        def _():
            step(True, True)

        @pl.when(i == heads)
        def _():
            step(False, True)

    out_shape = (sources, span_dev, width + HD)
    return pl.pallas_call(
        body,
        out_shape=jax.ShapeDtypeStruct(out_shape, jnp.bfloat16),
        grid_spec=pltpu.PrefetchScalarGridSpec(
            num_scalar_prefetch=1,
            grid=(heads + 1,),
            in_specs=[
                pl.BlockSpec(
                    (sources, span_dev, HD), lambda i, f: (0, 0, jnp.minimum(i, heads - 1))
                ),
                whole(cached, HD),
                whole(cached, HD),
                whole(fresh, HD),
                whole(fresh, HD),
                whole(1, span_dev, HD),
            ],
            out_specs=whole(*out_shape),
            scratch_shapes=[
                pltpu.VMEM((HD, total), jnp.bfloat16),
                pltpu.VMEM((total, 2 * HD), jnp.bfloat16),
                pltpu.VMEM((2, span, total), jnp.float32),
                pltpu.VMEM((2, span, HD), jnp.float32),
            ],
        ),
        compiler_params=pltpu.CompilerParams(
            dimension_semantics=("arbitrary",), vmem_limit_bytes=48 << 20
        ),
        cost_estimate=pl.CostEstimate(
            flops=4 * heads * span * total * HD,
            transcendentals=heads * span * total,
            bytes_accessed=6 << 20,
        ),
        name="attend",
    )(first_token, queries, keys, values, fresh_keys, fresh_values, side)


def merge(pieces, copies):
    sources, span_dev, wide = pieces.shape
    width = wide - HD
    heads = width // HD

    def body(in_ref, out_ref):
        tail = in_ref[:, :, width:].astype(jnp.float32).reshape(sources * span_dev, HD)
        level = (tail + pltpu.roll(tail, HD - heads, 1)).reshape(sources, span_dev, HD)
        top = jnp.max(level, axis=0)
        weight = jnp.exp2(level - top[None])
        weight = weight / jnp.sum(weight, axis=0)[None]
        for h in range(heads):
            cols = slice(h * HD, (h + 1) * HD)
            acc = None
            for k in range(sources):
                part = in_ref[k, :, cols].astype(jnp.float32) * weight[k][:, h : h + 1]
                acc = part if acc is None else acc + part
            acc = acc.astype(jnp.bfloat16)
            for k in range(copies):
                out_ref[k, :, cols] = acc

    return pl.pallas_call(
        body,
        out_shape=jax.ShapeDtypeStruct((copies, span_dev, width), jnp.bfloat16),
        in_specs=[whole(*pieces.shape)],
        out_specs=whole(copies, span_dev, width),
        grid=(1,),
        name="merge",
    )(pieces)


def score(chunks, places, inverse, own, partner, state, local_target):
    blocks, span, cols = chunks[0].shape
    count = len(chunks)
    vocab = own.shape[0]
    first, last = state is None, local_target is not None
    across = (((1,), (1,)), ((), ()))

    def body(*refs):
        refs = list(refs[1:])
        take = lambda n: [refs.pop(0) for _ in range(n)]
        x_refs, inv_refs, own_refs, partner_refs = (take(count) for _ in range(4))
        old = [] if first else take(2)
        t_ref = take(1)[0] if last else None
        acc, squares = (refs[1], refs[2]) if last else (refs[0], refs[1])
        i = pl.program_id(0)

        @pl.when(i == 0)
        def _():
            acc[...] = jnp.zeros_like(acc) if first else old[0][...]
            squares[...] = jnp.zeros_like(squares) if first else old[1][...]

        ss = None
        for side, w_refs in enumerate((own_refs, partner_refs)):
            total = None
            for x_ref, w_ref in zip(x_refs, w_refs):
                d = lax.dot_general(
                    w_ref[...], x_ref[0], across, preferred_element_type=jnp.float32
                )
                total = d if total is None else total + d
            acc[side] += total
        for x_ref, inv_ref in zip(x_refs, inv_refs):
            xf = x_ref[0].astype(jnp.float32)
            sq = xf * xf * inv_ref[0]
            for b in range(0, cols, 128):
                piece = sq[:, b : b + 128]
                ss = piece if ss is None else ss + piece
        squares[...] += ss

        if last:

            @pl.when(i == blocks - 1)
            def _():
                mean = jnp.sum(squares[...].T, axis=0, keepdims=True) / D
                scale = lax.rsqrt(mean + EPSILON)
                row = lax.broadcasted_iota(jnp.int32, (vocab, span), 0)
                logits = [acc[side] * scale for side in range(2)]
                top = jnp.max(jnp.maximum(*logits), axis=0, keepdims=True)
                sums = sum(
                    jnp.sum(jnp.exp(part - top), axis=0, keepdims=True) for part in logits
                )
                hit = sum(
                    jnp.sum(
                        jnp.where(row == t_ref[side : side + 1, :], logits[side], 0.0),
                        axis=0,
                        keepdims=True,
                    )
                    for side in range(2)
                )
                refs[0][...] = jnp.concatenate([top + jnp.log(sums), hit], 0)

    kept = [(2, vocab, span), (span, 128)]
    kept_shape = tuple(jax.ShapeDtypeStruct(k, jnp.float32) for k in kept)
    pick = lambda n: pl.BlockSpec((1, 1, cols), lambda i, at: (at[n, i], 0, 0))
    weigh = lambda n: pl.BlockSpec((vocab, cols), lambda i, at: (0, at[n, i]))
    in_specs = [pl.BlockSpec((1, span, cols), lambda i, at: (i, 0, 0))] * count
    in_specs += [pick(n) for n in range(count)]
    in_specs += [weigh(n) for n in range(count)] * 2
    operands = [*chunks, *[inverse] * count, *[own] * count, *[partner] * count]
    if not first:
        in_specs += [whole(*k) for k in kept]
        operands += state
    if last:
        in_specs.append(whole(2, span))
        operands.append(local_target)
        out_shape, out_specs = jax.ShapeDtypeStruct((2, span), jnp.float32), whole(2, span)
        scratch = [pltpu.VMEM(k, jnp.float32) for k in kept]
    else:
        out_shape, out_specs, scratch = kept_shape, tuple(whole(*k) for k in kept), []
    return pl.pallas_call(
        body,
        out_shape=out_shape,
        grid_spec=pltpu.PrefetchScalarGridSpec(
            num_scalar_prefetch=1,
            grid=(blocks,),
            in_specs=in_specs,
            out_specs=out_specs,
            scratch_shapes=scratch,
        ),
        compiler_params=pltpu.CompilerParams(
            dimension_semantics=("arbitrary",), vmem_limit_bytes=40 << 20
        ),
        cost_estimate=pl.CostEstimate(
            flops=4 * span * blocks * count * cols * vocab,
            transcendentals=2 * span * vocab if last else 0,
            bytes_accessed=4 * blocks * count * cols * vocab,
        ),
        name="score",
    )(places, *operands)


def shifted(value, axis, by):
    count = lax.axis_size(axis)
    return lax.ppermute(value, axis, [(i, (i + by) % count) for i in range(count)])


def local(
    queries,
    cache_keys,
    cache_values,
    span_keys,
    span_values,
    out_weight,
    residual,
    norm_gain,
    head_weight,
    targets,
    window_lengths,
):
    x, z = lax.axis_index("ctx_0"), lax.axis_index("ctx_1")
    y, core = lax.axis_index("tp_0"), lax.axis_index("tp_1")
    xs, zs, ys = (lax.axis_size(name) for name in ("ctx_0", "ctx_1", "tp_0"))
    ctx_rank = lax.axis_index(CTX)
    span_dev, width = queries.shape
    ctx_size = lax.axis_size(CTX)
    span_total = span_dev * ctx_size
    first_token = ctx_rank * span_dev
    model_dev = norm_gain.shape[0]
    own_weight = head_weight.T
    partner_weight = shifted(own_weight, "tp_1", 1)
    gain_lanes = model_dev // span_dev
    side = jnp.pad(
        norm_gain.reshape(1, span_dev, gain_lanes),
        ((0, 0), (0, 0), (2 * GROUP, HD - 2 * GROUP - gain_lanes)),
    )
    partial = attend(
        first_token.reshape(1),
        sent_to_all(queries, CTX),
        cache_keys,
        cache_values,
        span_keys,
        span_values,
        side,
    )
    pieces = lax.all_to_all(partial, CTX, split_axis=0, concat_axis=0, tiled=True)
    half = model_dev // 2
    gains = pieces[:, :, width + 2 * GROUP : width + 2 * GROUP + gain_lanes]
    gains = gains.reshape(2 * ctx_size, 1, half).astype(jnp.float32)
    inverse = 1.0 / (gains * gains)
    attended = lax.all_to_all(merge(pieces, ctx_size), CTX, split_axis=0, concat_axis=0, tiled=True)

    tokens = span_total // (2 * ys)
    by_core = attended.reshape(ys, 2, tokens, width)

    def projected(which):
        rows = lax.dynamic_index_in_dim(by_core, which, 1, keepdims=False)
        return jnp.dot(
            rows.reshape(ys * tokens, width), out_weight, preferred_element_type=jnp.float32
        )

    arrived = shifted(projected(1 - core).astype(jnp.bfloat16), "tp_1", 1)
    both = projected(core) + arrived.astype(jnp.float32)
    both = both.reshape(ys, tokens, model_dev)
    stream = residual.astype(jnp.float32) + lax.dynamic_index_in_dim(both, y, 0, keepdims=False)
    sent = both.astype(jnp.bfloat16)
    for by in range(1, ys):
        block = lax.dynamic_index_in_dim(sent, (y + by) % ys, 0, keepdims=False)
        stream = stream + shifted(block, "tp_0", by).astype(jnp.float32)
    gained = (stream * norm_gain.astype(jnp.float32)[None, :]).astype(jnp.bfloat16)
    rows = [gained] + [shifted(gained, "tp_0", by) for by in range(1, ys)]
    rows = jnp.concatenate(rows, 0)

    def places(steps, part):
        dx = jnp.array([s[0] for s in steps], jnp.int32)
        dz = jnp.array([s[1] for s in steps], jnp.int32)
        return 2 * (((x + dx) % xs) * zs + (z + dz) % zs) + part

    def gathered(value, first, second):
        behind, ahead = shifted(value, first, 1), shifted(value, first, -1)
        across = shifted(behind, first, 1)
        near = jnp.stack([value, behind, ahead, across])
        return near, (shifted(near, second, 1), shifted(near, second, -1))

    def forwarded(pair, second):
        return shifted(pair[0][:2], second, 1), shifted(pair[1][2:], second, -1)

    order = (0, -1, 1, -2)
    near_a, next_a = gathered(rows[:, :half], "ctx_1", "ctx_0")
    near_b, next_b = gathered(rows[:, half:], "ctx_0", "ctx_1")
    at_a = lambda step, among: places([(step, o) for o in among], 0)
    at_b = lambda step, among: places([(o, step) for o in among], 1)
    vocab_dev = head_weight.shape[1]
    mine = lax.dynamic_index_in_dim(targets.reshape(ys, 2, tokens), core, 1, keepdims=False)
    turn = (y - jnp.arange(ys, dtype=jnp.int32)) % ys
    turned = turn[:, None] == jnp.arange(ys, dtype=jnp.int32)[None, :]
    mine = jnp.sum(jnp.where(turned[:, :, None], mine[None], 0), axis=1).reshape(1, -1)
    rank = lax.axis_index(CTX_TP)
    starts = jnp.stack([rank, rank + 1 - 2 * core]) * vocab_dev
    local_target = mine - starts[:, None]
    state = score(
        (near_a, near_b),
        jnp.stack([at_a(0, order), at_b(0, order)]),
        inverse,
        own_weight,
        partner_weight,
        None,
        None,
    )
    next_a, next_b, state = lax.optimization_barrier((next_a, next_b, state))
    far_a, far_b = forwarded(next_a, "ctx_0"), forwarded(next_b, "ctx_1")
    state = score(
        (*next_a, *next_b),
        jnp.stack([at_a(-1, order), at_a(1, order), at_b(-1, order), at_b(1, order)]),
        inverse,
        own_weight,
        partner_weight,
        state,
        None,
    )
    level_hit = score(
        (*far_a, *far_b),
        jnp.stack(
            [at_a(-2, order[:2]), at_a(-2, order[2:]), at_b(-2, order[:2]), at_b(-2, order[2:])]
        ),
        inverse,
        own_weight,
        partner_weight,
        state,
        local_target,
    )
    level_hit = level_hit.reshape(2, ys, 1, tokens)
    level_hit = jnp.sum(jnp.where(turned.T[None, :, :, None], level_hit.reshape(2, 1, ys, tokens), 0.0), axis=2)
    gathered_stats = sent_to_all(level_hit.reshape(2, ys * tokens), ("ctx_0", "ctx_1", "tp_0"))
    level, hit = gathered_stats[:, 0], gathered_stats[:, 1]
    top = jnp.max(level, axis=0)
    total = top + jnp.log(jnp.sum(jnp.exp(level - top[None]), axis=0))
    my_logprob = jnp.sum(hit, axis=0) - total
    other_logprob = shifted(my_logprob, "tp_1", 1)
    pair = jnp.stack([my_logprob.reshape(ys, tokens), other_logprob.reshape(ys, tokens)], 1)
    token_logprob = jnp.where(core == 0, pair, pair[:, ::-1]).reshape(span_total)
    window_ends = jnp.cumsum(window_lengths)
    window_starts = window_ends - window_lengths
    positions = jnp.arange(span_total, dtype=jnp.int32)
    member = (positions[None, :] >= window_starts[:, None]) & (
        positions[None, :] < window_ends[:, None]
    )
    window_sums = jnp.sum(jnp.where(member, token_logprob[None, :], 0.0), axis=1)
    window_means = window_sums / window_lengths.astype(jnp.float32)
    own_logprob = lax.dynamic_slice_in_dim(token_logprob, first_token, span_dev, 0)
    return (own_logprob, window_means)


def solution(mesh):
    split = Mesh(mesh.devices.reshape(4, 4, 4, 2), ("ctx_0", "ctx_1", "tp_0", "tp_1"))
    in_specs = (
        P(CTX, TP),
        P(CTX, TP),
        P(CTX, TP),
        P(CTX, TP),
        P(CTX, TP),
        P(TP, CTX),
        P(TP, CTX),
        P(CTX),
        P(None, CTX_TP),
        P(),
        P(),
    )
    out_specs = (P(CTX), P())
    return jax.shard_map(local, mesh=split, in_specs=in_specs, out_specs=out_specs, check_vma=False)
```

```python
import jax
import jax.numpy as jnp
from jax import lax
from jax.experimental import pallas as pl
from jax.experimental.pallas import tpu as pltpu
from jax.sharding import Mesh
from jax.sharding import PartitionSpec as P

D = 8192
HEADS = 64
KV_HEADS = 8
HD = 128
GROUP = HEADS // KV_HEADS
CTX = ("ctx_0", "ctx_1")
TP = ("tp_0", "tp_1")
CTX_TP = ("ctx_0", "ctx_1", "tp_0", "tp_1")
EPSILON = 1e-05
NEGATIVE = -1e30
LOG2E = 1.4426950408889634
TO_LOG2 = HD ** (-0.5) * LOG2E
ROWS = 256
KEYS = 2048
MERGE_ROWS = 16


def sent_to_all(value, axis):
    count = lax.axis_size(axis)
    return lax.all_to_all(
        jnp.broadcast_to(value[None], (count, *value.shape)), axis, 0, 0, tiled=True
    )


def whole(*shape):
    return pl.BlockSpec(shape, lambda *at: (0,) * len(shape))


def attend(first_token, queries, keys, values, fresh_keys, fresh_values, side):
    sources, span_dev, width = queries.shape
    span, cached, fresh = sources * span_dev, keys.shape[0], fresh_keys.shape[0]
    heads = width // HD
    total = cached + 128
    chunks = [(a, KEYS) for a in range(0, cached, KEYS)]
    chunks[-1] = (chunks[-1][0], total - chunks[-1][0])

    def body(first_ref, q_ref, k_ref, v_ref, fk_ref, fv_ref, side_ref, out_ref, kt, va, sbuf, mbuf):
        i = pl.program_id(0)

        @pl.when(i == 0)
        def _():
            for a in range(0, cached, 512):
                kt[:, a : a + 512] = k_ref[a : a + 512, :].T
            gap = jnp.zeros((128 - fresh, HD), jnp.bfloat16)
            kt[:, cached:] = jnp.concatenate([fk_ref[...], gap], 0).T
            va[:cached, :HD] = v_ref[...]
            va[cached:, :HD] = jnp.concatenate([fv_ref[...], gap], 0)
            va[:, HD:] = jnp.ones((total, HD), jnp.bfloat16)
            out_ref[:, :, width:] = jnp.broadcast_to(side_ref[...], (sources, span_dev, HD))

        def step(scoring, weighing):
            to = lax.rem(i, 2)
            at = lax.rem(i + 1, 2)
            for r in range(0, span, ROWS):
                rows = slice(r, r + ROWS)
                tokens = slice(r // span_dev, (r + ROWS) // span_dev)
                top, acc = None, None
                if scoring:
                    q = q_ref[tokens].reshape(ROWS, HD)
                if weighing:
                    shift = mbuf[at, rows, :]
                for a, n in chunks:
                    if scoring:
                        s = jnp.dot(q, kt[:, a : a + n], preferred_element_type=jnp.float32)
                        if a + n == total:
                            col = lax.broadcasted_iota(jnp.int32, (ROWS, 128), 1)
                            row = lax.broadcasted_iota(jnp.int32, (ROWS, 128), 0) + r
                            seen = (col < fresh) & (row >= col + first_ref[0])
                            tail = jnp.where(seen, s[:, n - 128 :], NEGATIVE)
                            s = jnp.concatenate([s[:, : n - 128], tail], 1)
                        sbuf[to, rows, a : a + n] = s
                        for b in range(0, n, 128):
                            piece = s[:, b : b + 128]
                            top = piece if top is None else jnp.maximum(top, piece)
                    if weighing:
                        p = jnp.concatenate(
                            [
                                jnp.exp2(
                                    sbuf[at, rows, a + b : a + b + 128] * TO_LOG2 - shift
                                ).astype(jnp.bfloat16)
                                for b in range(0, n, 128)
                            ],
                            1,
                        )
                        d = jnp.dot(p, va[a : a + n, :], preferred_element_type=jnp.float32)
                        acc = d if acc is None else acc + d
                if scoring:
                    m = jnp.max(top, axis=1, keepdims=True) * TO_LOG2
                    mbuf[to, rows, :] = jnp.broadcast_to(m, (ROWS, 128))
                if weighing:
                    h = i - 1
                    row_sum = acc[:, HD:]
                    o = (acc[:, :HD] / row_sum).astype(jnp.bfloat16)
                    place = pl.ds(pl.multiple_of(h * HD, HD), HD)
                    out_ref[tokens, :, place] = o.reshape(-1, span_dev, HD)
                    level = shift + jnp.log2(row_sum)
                    high = level.astype(jnp.bfloat16).astype(jnp.float32)
                    low = level - high
                    lane = lax.broadcasted_iota(jnp.int32, (ROWS, HD), 1)
                    old = out_ref[tokens, :, width:].reshape(ROWS, HD).astype(jnp.float32)
                    new = jnp.where(lane == h, high, jnp.where(lane == h + heads, low, old))
                    out_ref[tokens, :, width:] = new.astype(jnp.bfloat16).reshape(-1, span_dev, HD)

        @pl.when(i == 0)
        def _():
            step(True, False)

        @pl.when((i > 0) & (i < heads))
        def _():
            step(True, True)

        @pl.when(i == heads)
        def _():
            step(False, True)

    out_shape = (sources, span_dev, width + HD)
    return pl.pallas_call(
        body,
        out_shape=jax.ShapeDtypeStruct(out_shape, jnp.bfloat16),
        grid_spec=pltpu.PrefetchScalarGridSpec(
            num_scalar_prefetch=1,
            grid=(heads + 1,),
            in_specs=[
                pl.BlockSpec(
                    (sources, span_dev, HD), lambda i, f: (0, 0, jnp.minimum(i, heads - 1))
                ),
                whole(cached, HD),
                whole(cached, HD),
                whole(fresh, HD),
                whole(fresh, HD),
                whole(1, span_dev, HD),
            ],
            out_specs=whole(*out_shape),
            scratch_shapes=[
                pltpu.VMEM((HD, total), jnp.bfloat16),
                pltpu.VMEM((total, 2 * HD), jnp.bfloat16),
                pltpu.VMEM((2, span, total), jnp.float32),
                pltpu.VMEM((2, span, HD), jnp.float32),
            ],
        ),
        compiler_params=pltpu.CompilerParams(
            dimension_semantics=("arbitrary",), vmem_limit_bytes=30 << 20
        ),
        cost_estimate=pl.CostEstimate(
            flops=4 * heads * span * total * HD,
            transcendentals=heads * span * total,
            bytes_accessed=6 << 20,
        ),
        name="attend",
    )(first_token, queries, keys, values, fresh_keys, fresh_values, side)


def merge(pieces, copies):
    sources, span_dev, wide = pieces.shape
    width = wide - HD
    heads = width // HD
    rows = MERGE_ROWS

    def body(in_ref, out_ref):
        tail = in_ref[:, :, width:].astype(jnp.float32).reshape(sources * rows, HD)
        level = (tail + pltpu.roll(tail, HD - heads, 1)).reshape(sources, rows, HD)
        top = jnp.max(level, axis=0)
        weight = jnp.exp2(level - top[None])
        weight = weight / jnp.sum(weight, axis=0)[None]
        for h in range(heads):
            cols = slice(h * HD, (h + 1) * HD)
            acc = None
            for k in range(sources):
                part = in_ref[k, :, cols].astype(jnp.float32) * weight[k][:, h : h + 1]
                acc = part if acc is None else acc + part
            acc = acc.astype(jnp.bfloat16)
            for k in range(copies):
                out_ref[k, :, cols] = acc

    return pl.pallas_call(
        body,
        out_shape=jax.ShapeDtypeStruct((copies, span_dev, width), jnp.bfloat16),
        in_specs=[pl.BlockSpec((sources, rows, wide), lambda i: (0, i, 0))],
        out_specs=pl.BlockSpec((copies, rows, width), lambda i: (0, i, 0)),
        grid=(span_dev // rows,),
        compiler_params=pltpu.CompilerParams(vmem_limit_bytes=10 << 20),
        name="merge",
    )(pieces)


def score(chunks, places, inverse, own, partner, state, local_target):
    blocks, span, cols = chunks[0].shape
    count = len(chunks)
    vocab = own.shape[0]
    first, last = state is None, local_target is not None
    across = (((1,), (1,)), ((), ()))

    def body(*refs):
        at_ref, *refs = refs
        take = lambda n: [refs.pop(0) for _ in range(n)]
        x_refs, inv_ref = take(count), take(1)[0]
        own_refs, partner_refs = take(count), take(count)
        old = [] if first else take(2)
        t_ref = take(1)[0] if last else None
        acc, squares = (refs[1], refs[2]) if last else (refs[0], refs[1])
        i = pl.program_id(0)

        @pl.when(i == 0)
        def _():
            acc[...] = jnp.zeros_like(acc) if first else old[0][...]
            squares[...] = jnp.zeros_like(squares) if first else old[1][...]

        ss = None
        parts = [x_ref[i] for x_ref in x_refs]
        joint = jnp.concatenate(parts, 1)
        for side, w_refs in enumerate((own_refs, partner_refs)):
            w = jnp.concatenate([w_ref[...] for w_ref in w_refs], 1)
            acc[side] += lax.dot_general(w, joint, across, preferred_element_type=jnp.float32)
        for n, part in enumerate(parts):
            xf = part.astype(jnp.float32)
            sq = xf * xf * inv_ref[at_ref[n, i]]
            for b in range(0, cols, 128):
                piece = sq[:, b : b + 128]
                ss = piece if ss is None else ss + piece
        squares[...] += ss

        if last:

            @pl.when(i == blocks - 1)
            def _():
                mean = jnp.sum(squares[...].T, axis=0, keepdims=True) / D
                scale = lax.rsqrt(mean + EPSILON)
                row = lax.broadcasted_iota(jnp.int32, (vocab, span), 0)
                logits = [acc[side] * scale for side in range(2)]
                top = jnp.max(jnp.maximum(*logits), axis=0, keepdims=True)
                sums = sum(
                    jnp.sum(jnp.exp(part - top), axis=0, keepdims=True) for part in logits
                )
                hit = sum(
                    jnp.sum(
                        jnp.where(row == t_ref[side : side + 1, :], logits[side], 0.0),
                        axis=0,
                        keepdims=True,
                    )
                    for side in range(2)
                )
                refs[0][...] = jnp.concatenate([top + jnp.log(sums), hit], 0)

    kept = [(2, vocab, span), (span, 128)]
    kept_shape = tuple(jax.ShapeDtypeStruct(k, jnp.float32) for k in kept)
    weigh = lambda n: pl.BlockSpec((vocab, cols), lambda i, at: (0, at[n, i]))
    in_specs = [whole(*chunk.shape) for chunk in chunks] + [whole(*inverse.shape)]
    in_specs += [weigh(n) for n in range(count)] * 2
    operands = [*chunks, inverse, *[own] * count, *[partner] * count]
    if not first:
        in_specs += [whole(*k) for k in kept]
        operands += state
    if last:
        in_specs.append(whole(2, span))
        operands.append(local_target)
        out_shape, out_specs = jax.ShapeDtypeStruct((2, span), jnp.float32), whole(2, span)
        scratch = [pltpu.VMEM(k, jnp.float32) for k in kept]
    else:
        out_shape, out_specs, scratch = kept_shape, tuple(whole(*k) for k in kept), []
    return pl.pallas_call(
        body,
        out_shape=out_shape,
        grid_spec=pltpu.PrefetchScalarGridSpec(
            num_scalar_prefetch=1,
            grid=(blocks,),
            in_specs=in_specs,
            out_specs=out_specs,
            scratch_shapes=scratch,
        ),
        compiler_params=pltpu.CompilerParams(
            dimension_semantics=("arbitrary",), vmem_limit_bytes=24 << 20
        ),
        cost_estimate=pl.CostEstimate(
            flops=4 * span * blocks * count * cols * vocab,
            transcendentals=2 * span * vocab if last else 0,
            bytes_accessed=4 * blocks * count * cols * vocab,
        ),
        name="score",
    )(places, *operands)


def shifted(value, axis, by):
    count = lax.axis_size(axis)
    return lax.ppermute(value, axis, [(i, (i + by) % count) for i in range(count)])


def local(
    queries,
    cache_keys,
    cache_values,
    span_keys,
    span_values,
    out_weight,
    residual,
    norm_gain,
    head_weight,
    targets,
    window_lengths,
):
    x, z = lax.axis_index("ctx_0"), lax.axis_index("ctx_1")
    y, core = lax.axis_index("tp_0"), lax.axis_index("tp_1")
    xs, zs, ys = (lax.axis_size(name) for name in ("ctx_0", "ctx_1", "tp_0"))
    ctx_rank = lax.axis_index(CTX)
    span_dev, width = queries.shape
    ctx_size = lax.axis_size(CTX)
    span_total = span_dev * ctx_size
    first_token = ctx_rank * span_dev
    model_dev = norm_gain.shape[0]
    own_weight = head_weight.T
    partner_weight = shifted(own_weight, "tp_1", 1)
    gain_lanes = model_dev // span_dev
    side = jnp.pad(
        norm_gain.reshape(1, span_dev, gain_lanes),
        ((0, 0), (0, 0), (2 * GROUP, HD - 2 * GROUP - gain_lanes)),
    )
    partial = attend(
        first_token.reshape(1),
        sent_to_all(queries, CTX),
        cache_keys,
        cache_values,
        span_keys,
        span_values,
        side,
    )
    pieces = lax.all_to_all(partial, CTX, split_axis=0, concat_axis=0, tiled=True)
    half = model_dev // 2
    gains = pieces[:, :, width + 2 * GROUP : width + 2 * GROUP + gain_lanes]
    gains = gains.reshape(2 * ctx_size, 1, half).astype(jnp.float32)
    inverse = 1.0 / (gains * gains)
    attended = lax.all_to_all(merge(pieces, ctx_size), CTX, split_axis=0, concat_axis=0, tiled=True)

    tokens = span_total // (2 * ys)
    by_core = attended.reshape(ys, 2, tokens, width)

    def projected(which):
        rows = lax.dynamic_index_in_dim(by_core, which, 1, keepdims=False)
        return jnp.dot(
            rows.reshape(ys * tokens, width), out_weight, preferred_element_type=jnp.float32
        )

    arrived = shifted(projected(1 - core).astype(jnp.bfloat16), "tp_1", 1)
    both = projected(core) + arrived.astype(jnp.float32)
    both = both.reshape(ys, tokens, model_dev)
    stream = residual.astype(jnp.float32) + lax.dynamic_index_in_dim(both, y, 0, keepdims=False)
    sent = both.astype(jnp.bfloat16)
    for by in range(1, ys):
        block = lax.dynamic_index_in_dim(sent, (y + by) % ys, 0, keepdims=False)
        stream = stream + shifted(block, "tp_0", by).astype(jnp.float32)
    gained = (stream * norm_gain.astype(jnp.float32)[None, :]).astype(jnp.bfloat16)
    rows = [gained] + [shifted(gained, "tp_0", by) for by in range(1, ys)]
    rows = jnp.concatenate(rows, 0)

    def places(steps, part):
        dx = jnp.array([s[0] for s in steps], jnp.int32)
        dz = jnp.array([s[1] for s in steps], jnp.int32)
        return 2 * (((x + dx) % xs) * zs + (z + dz) % zs) + part

    def gathered(value, first, second):
        behind, ahead = shifted(value, first, 1), shifted(value, first, -1)
        across = shifted(behind, first, 1)
        near = jnp.stack([value, behind, ahead, across])
        return near, (shifted(near, second, 1), shifted(near, second, -1))

    order = (0, -1, 1, -2)
    near_a, next_a = gathered(rows[:, :half], "ctx_1", "ctx_0")
    near_b, next_b = gathered(rows[:, half:], "ctx_0", "ctx_1")
    at_a = lambda step, among: places([(step, o) for o in among], 0)
    at_b = lambda step, among: places([(o, step) for o in among], 1)
    vocab_dev = head_weight.shape[1]
    mine = lax.dynamic_index_in_dim(targets.reshape(ys, 2, tokens), core, 1, keepdims=False)
    turn = (y - jnp.arange(ys, dtype=jnp.int32)) % ys
    turned = turn[:, None] == jnp.arange(ys, dtype=jnp.int32)[None, :]
    mine = jnp.sum(jnp.where(turned[:, :, None], mine[None], 0), axis=1).reshape(1, -1)
    rank = lax.axis_index(CTX_TP)
    starts = jnp.stack([rank, rank + 1 - 2 * core]) * vocab_dev
    local_target = mine - starts[:, None]
    state = score(
        (near_a, near_b),
        jnp.stack([at_a(0, order), at_b(0, order)]),
        inverse,
        own_weight,
        partner_weight,
        None,
        None,
    )
    next_a, next_b, state = lax.optimization_barrier((next_a, next_b, state))
    far_a, far_b = shifted(next_a[0], "ctx_0", 1), shifted(next_b[0], "ctx_1", 1)
    state = score(
        (*next_a, *next_b),
        jnp.stack([at_a(-1, order), at_a(1, order), at_b(-1, order), at_b(1, order)]),
        inverse,
        own_weight,
        partner_weight,
        state,
        None,
    )
    level_hit = score(
        (far_a, far_b),
        jnp.stack([at_a(-2, order), at_b(-2, order)]),
        inverse,
        own_weight,
        partner_weight,
        state,
        local_target,
    )
    level_hit = level_hit.reshape(2, ys, 1, tokens)
    level_hit = jnp.sum(jnp.where(turned.T[None, :, :, None], level_hit.reshape(2, 1, ys, tokens), 0.0), axis=2)
    gathered_stats = sent_to_all(level_hit.reshape(2, ys * tokens), ("ctx_0", "ctx_1", "tp_0"))
    level, hit = gathered_stats[:, 0], gathered_stats[:, 1]
    top = jnp.max(level, axis=0)
    total = top + jnp.log(jnp.sum(jnp.exp(level - top[None]), axis=0))
    my_logprob = jnp.sum(hit, axis=0) - total
    other_logprob = shifted(my_logprob, "tp_1", 1)
    pair = jnp.stack([my_logprob.reshape(ys, tokens), other_logprob.reshape(ys, tokens)], 1)
    token_logprob = jnp.where(core == 0, pair, pair[:, ::-1]).reshape(span_total)
    window_ends = jnp.cumsum(window_lengths)
    window_starts = window_ends - window_lengths
    positions = jnp.arange(span_total, dtype=jnp.int32)
    member = (positions[None, :] >= window_starts[:, None]) & (
        positions[None, :] < window_ends[:, None]
    )
    window_sums = jnp.sum(jnp.where(member, token_logprob[None, :], 0.0), axis=1)
    window_means = window_sums / window_lengths.astype(jnp.float32)
    own_logprob = lax.dynamic_slice_in_dim(token_logprob, first_token, span_dev, 0)
    return (own_logprob, window_means)


def solution(mesh):
    split = Mesh(mesh.devices.reshape(4, 4, 4, 2), ("ctx_0", "ctx_1", "tp_0", "tp_1"))
    in_specs = (
        P(CTX, TP),
        P(CTX, TP),
        P(CTX, TP),
        P(CTX, TP),
        P(CTX, TP),
        P(TP, CTX),
        P(TP, CTX),
        P(CTX),
        P(None, CTX_TP),
        P(),
        P(),
    )
    out_specs = (P(CTX), P())
    return jax.shard_map(local, mesh=split, in_specs=in_specs, out_specs=out_specs, check_vma=False)
```

```python
import jax
import jax.numpy as jnp
from jax import lax
from jax.experimental import pallas as pl
from jax.experimental.pallas import tpu as pltpu
from jax.sharding import Mesh
from jax.sharding import PartitionSpec as P

D = 8192
HEADS = 64
KV_HEADS = 8
HD = 128
GROUP = HEADS // KV_HEADS
CTX = ("ctx_0", "ctx_1")
TP = ("tp_0", "tp_1")
CTX_TP = ("ctx_0", "ctx_1", "tp_0", "tp_1")
EPSILON = 1e-05
NEGATIVE = -1e30
LOG2E = 1.4426950408889634
TO_LOG2 = HD ** (-0.5) * LOG2E
ROWS = 256
KEYS = 2048
MERGE_ROWS = 16


def sent_to_all(value, axis):
    count = lax.axis_size(axis)
    return lax.all_to_all(
        jnp.broadcast_to(value[None], (count, *value.shape)), axis, 0, 0, tiled=True
    )


def whole(*shape):
    return pl.BlockSpec(shape, lambda *at: (0,) * len(shape))


def copies_of(value, count):
    def body(in_ref, out_ref, sems):
        moves = [
            pltpu.make_async_copy(in_ref, out_ref.at[k], sems.at[k]) for k in range(count)
        ]
        for move in moves:
            move.start()
        for move in moves:
            move.wait()

    return pl.pallas_call(
        body,
        out_shape=jax.ShapeDtypeStruct((count, *value.shape), value.dtype),
        in_specs=[whole(*value.shape)],
        out_specs=pl.BlockSpec(memory_space=pl.ANY),
        grid=(1,),
        scratch_shapes=[pltpu.SemaphoreType.DMA((count,))],
        compiler_params=pltpu.CompilerParams(vmem_limit_bytes=2 << 20),
        name="spread",
    )(value)


def attend(first_token, queries, keys, values, fresh_keys, fresh_values, side):
    sources, span_dev, width = queries.shape
    span, cached, fresh = sources * span_dev, keys.shape[0], fresh_keys.shape[0]
    heads = width // HD
    total = cached + 128
    chunks = [(a, KEYS) for a in range(0, cached, KEYS)]
    chunks[-1] = (chunks[-1][0], total - chunks[-1][0])

    def body(first_ref, q_ref, k_ref, v_ref, fk_ref, fv_ref, side_ref, out_ref, kt, va, sbuf, mbuf):
        i = pl.program_id(0)

        @pl.when(i == 0)
        def _():
            for a in range(0, cached, 512):
                kt[:, a : a + 512] = k_ref[a : a + 512, :].T
            gap = jnp.zeros((128 - fresh, HD), jnp.bfloat16)
            kt[:, cached:] = jnp.concatenate([fk_ref[...], gap], 0).T
            va[:cached, :HD] = v_ref[...]
            va[cached:, :HD] = jnp.concatenate([fv_ref[...], gap], 0)
            va[:, HD:] = jnp.ones((total, HD), jnp.bfloat16)
            out_ref[:, :, width:] = jnp.broadcast_to(side_ref[...], (sources, span_dev, HD))

        def step(scoring, weighing):
            to = lax.rem(i, 2)
            at = lax.rem(i + 1, 2)
            for r in range(0, span, ROWS):
                rows = slice(r, r + ROWS)
                tokens = slice(r // span_dev, (r + ROWS) // span_dev)
                top, acc = None, None
                if scoring:
                    q = q_ref[tokens].reshape(ROWS, HD)
                if weighing:
                    shift = mbuf[at, rows, :]
                for a, n in chunks:
                    if scoring:
                        s = jnp.dot(q, kt[:, a : a + n], preferred_element_type=jnp.float32)
                        if a + n == total:
                            col = lax.broadcasted_iota(jnp.int32, (ROWS, 128), 1)
                            row = lax.broadcasted_iota(jnp.int32, (ROWS, 128), 0) + r
                            seen = (col < fresh) & (row >= col + first_ref[0])
                            tail = jnp.where(seen, s[:, n - 128 :], NEGATIVE)
                            s = jnp.concatenate([s[:, : n - 128], tail], 1)
                        sbuf[to, rows, a : a + n] = s
                        for b in range(0, n, 128):
                            piece = s[:, b : b + 128]
                            top = piece if top is None else jnp.maximum(top, piece)
                    if weighing:
                        p = jnp.concatenate(
                            [
                                jnp.exp2(
                                    sbuf[at, rows, a + b : a + b + 128] * TO_LOG2 - shift
                                ).astype(jnp.bfloat16)
                                for b in range(0, n, 128)
                            ],
                            1,
                        )
                        d = jnp.dot(p, va[a : a + n, :], preferred_element_type=jnp.float32)
                        acc = d if acc is None else acc + d
                if scoring:
                    m = jnp.max(top, axis=1, keepdims=True) * TO_LOG2
                    mbuf[to, rows, :] = jnp.broadcast_to(m, (ROWS, 128))
                if weighing:
                    h = i - 1
                    row_sum = acc[:, HD:]
                    o = (acc[:, :HD] / row_sum).astype(jnp.bfloat16)
                    place = pl.ds(pl.multiple_of(h * HD, HD), HD)
                    out_ref[tokens, :, place] = o.reshape(-1, span_dev, HD)
                    level = shift + jnp.log2(row_sum)
                    high = level.astype(jnp.bfloat16).astype(jnp.float32)
                    low = level - high
                    lane = lax.broadcasted_iota(jnp.int32, (ROWS, HD), 1)
                    old = out_ref[tokens, :, width:].reshape(ROWS, HD).astype(jnp.float32)
                    new = jnp.where(lane == h, high, jnp.where(lane == h + heads, low, old))
                    out_ref[tokens, :, width:] = new.astype(jnp.bfloat16).reshape(-1, span_dev, HD)

        @pl.when(i == 0)
        def _():
            step(True, False)

        @pl.when((i > 0) & (i < heads))
        def _():
            step(True, True)

        @pl.when(i == heads)
        def _():
            step(False, True)

    out_shape = (sources, span_dev, width + HD)
    return pl.pallas_call(
        body,
        out_shape=jax.ShapeDtypeStruct(out_shape, jnp.bfloat16),
        grid_spec=pltpu.PrefetchScalarGridSpec(
            num_scalar_prefetch=1,
            grid=(heads + 1,),
            in_specs=[
                pl.BlockSpec(
                    (sources, span_dev, HD), lambda i, f: (0, 0, jnp.minimum(i, heads - 1))
                ),
                whole(cached, HD),
                whole(cached, HD),
                whole(fresh, HD),
                whole(fresh, HD),
                whole(1, span_dev, HD),
            ],
            out_specs=whole(*out_shape),
            scratch_shapes=[
                pltpu.VMEM((HD, total), jnp.bfloat16),
                pltpu.VMEM((total, 2 * HD), jnp.bfloat16),
                pltpu.VMEM((2, span, total), jnp.float32),
                pltpu.VMEM((2, span, HD), jnp.float32),
            ],
        ),
        compiler_params=pltpu.CompilerParams(
            dimension_semantics=("arbitrary",), vmem_limit_bytes=30 << 20
        ),
        cost_estimate=pl.CostEstimate(
            flops=4 * heads * span * total * HD,
            transcendentals=heads * span * total,
            bytes_accessed=6 << 20,
        ),
        name="attend",
    )(first_token, queries, keys, values, fresh_keys, fresh_values, side)


def merge(pieces, copies):
    sources, span_dev, wide = pieces.shape
    width = wide - HD
    heads = width // HD
    rows = MERGE_ROWS

    def body(in_ref, out_ref):
        tail = in_ref[:, :, width:].astype(jnp.float32).reshape(sources * rows, HD)
        level = (tail + pltpu.roll(tail, HD - heads, 1)).reshape(sources, rows, HD)
        top = jnp.max(level, axis=0)
        weight = jnp.exp2(level - top[None])
        weight = weight / jnp.sum(weight, axis=0)[None]
        for h in range(heads):
            cols = slice(h * HD, (h + 1) * HD)
            acc = None
            for k in range(sources):
                part = in_ref[k, :, cols].astype(jnp.float32) * weight[k][:, h : h + 1]
                acc = part if acc is None else acc + part
            acc = acc.astype(jnp.bfloat16)
            for k in range(copies):
                out_ref[k, :, cols] = acc

    return pl.pallas_call(
        body,
        out_shape=jax.ShapeDtypeStruct((copies, span_dev, width), jnp.bfloat16),
        in_specs=[pl.BlockSpec((sources, rows, wide), lambda i: (0, i, 0))],
        out_specs=pl.BlockSpec((copies, rows, width), lambda i: (0, i, 0)),
        grid=(span_dev // rows,),
        compiler_params=pltpu.CompilerParams(vmem_limit_bytes=10 << 20),
        name="merge",
    )(pieces)


def score(chunks, places, inverse, own, partner, state, local_target):
    blocks, span, cols = chunks[0].shape
    count = len(chunks)
    vocab = own.shape[0]
    first, last = state is None, local_target is not None
    across = (((1,), (1,)), ((), ()))

    def body(*refs):
        at_ref, *refs = refs
        take = lambda n: [refs.pop(0) for _ in range(n)]
        x_refs, inv_ref = take(count), take(1)[0]
        own_refs, partner_refs = take(count), take(count)
        old = [] if first else take(2)
        t_ref = take(1)[0] if last else None
        acc, squares = (refs[1], refs[2]) if last else (refs[0], refs[1])
        i = pl.program_id(0)

        @pl.when(i == 0)
        def _():
            acc[...] = jnp.zeros_like(acc) if first else old[0][...]
            squares[...] = jnp.zeros_like(squares) if first else old[1][...]

        ss = None
        parts = [x_ref[i] for x_ref in x_refs]
        joint = jnp.concatenate(parts, 1)
        for side, w_refs in enumerate((own_refs, partner_refs)):
            w = jnp.concatenate([w_ref[...] for w_ref in w_refs], 1)
            acc[side] += lax.dot_general(w, joint, across, preferred_element_type=jnp.float32)
        for n, part in enumerate(parts):
            xf = part.astype(jnp.float32)
            sq = xf * xf * inv_ref[at_ref[n, i]]
            for b in range(0, cols, 128):
                piece = sq[:, b : b + 128]
                ss = piece if ss is None else ss + piece
        squares[...] += ss

        if last:

            @pl.when(i == blocks - 1)
            def _():
                mean = jnp.sum(squares[...].T, axis=0, keepdims=True) / D
                scale = lax.rsqrt(mean + EPSILON)
                row = lax.broadcasted_iota(jnp.int32, (vocab, span), 0)
                logits = [acc[side] * scale for side in range(2)]
                top = jnp.max(jnp.maximum(*logits), axis=0, keepdims=True)
                sums = sum(
                    jnp.sum(jnp.exp(part - top), axis=0, keepdims=True) for part in logits
                )
                hit = sum(
                    jnp.sum(
                        jnp.where(row == t_ref[side : side + 1, :], logits[side], 0.0),
                        axis=0,
                        keepdims=True,
                    )
                    for side in range(2)
                )
                refs[0][...] = jnp.concatenate([top + jnp.log(sums), hit], 0)

    kept = [(2, vocab, span), (span, 128)]
    kept_shape = tuple(jax.ShapeDtypeStruct(k, jnp.float32) for k in kept)
    weigh = lambda n: pl.BlockSpec((vocab, cols), lambda i, at: (0, at[n, i]))
    in_specs = [whole(*chunk.shape) for chunk in chunks] + [whole(*inverse.shape)]
    in_specs += [weigh(n) for n in range(count)] * 2
    operands = [*chunks, inverse, *[own] * count, *[partner] * count]
    if not first:
        in_specs += [whole(*k) for k in kept]
        operands += state
    if last:
        in_specs.append(whole(2, span))
        operands.append(local_target)
        out_shape, out_specs = jax.ShapeDtypeStruct((2, span), jnp.float32), whole(2, span)
        scratch = [pltpu.VMEM(k, jnp.float32) for k in kept]
    else:
        out_shape, out_specs, scratch = kept_shape, tuple(whole(*k) for k in kept), []
    return pl.pallas_call(
        body,
        out_shape=out_shape,
        grid_spec=pltpu.PrefetchScalarGridSpec(
            num_scalar_prefetch=1,
            grid=(blocks,),
            in_specs=in_specs,
            out_specs=out_specs,
            scratch_shapes=scratch,
        ),
        compiler_params=pltpu.CompilerParams(
            dimension_semantics=("arbitrary",), vmem_limit_bytes=40 << 20
        ),
        cost_estimate=pl.CostEstimate(
            flops=4 * span * blocks * count * cols * vocab,
            transcendentals=2 * span * vocab if last else 0,
            bytes_accessed=4 * blocks * count * cols * vocab,
        ),
        name="score",
    )(places, *operands)


def shifted(value, axis, by):
    count = lax.axis_size(axis)
    return lax.ppermute(value, axis, [(i, (i + by) % count) for i in range(count)])


def local(
    queries,
    cache_keys,
    cache_values,
    span_keys,
    span_values,
    out_weight,
    residual,
    norm_gain,
    head_weight,
    targets,
    window_lengths,
):
    x, z = lax.axis_index("ctx_0"), lax.axis_index("ctx_1")
    y, core = lax.axis_index("tp_0"), lax.axis_index("tp_1")
    xs, zs, ys = (lax.axis_size(name) for name in ("ctx_0", "ctx_1", "tp_0"))
    ctx_rank = lax.axis_index(CTX)
    span_dev, width = queries.shape
    ctx_size = lax.axis_size(CTX)
    span_total = span_dev * ctx_size
    first_token = ctx_rank * span_dev
    model_dev = norm_gain.shape[0]
    own_weight = head_weight.T
    partner_weight = shifted(own_weight, "tp_1", 1)
    gain_lanes = model_dev // span_dev
    side = jnp.pad(
        norm_gain.reshape(1, span_dev, gain_lanes),
        ((0, 0), (0, 0), (2 * GROUP, HD - 2 * GROUP - gain_lanes)),
    )
    partial = attend(
        first_token.reshape(1),
        lax.all_to_all(copies_of(queries, ctx_size), CTX, 0, 0, tiled=True),
        cache_keys,
        cache_values,
        span_keys,
        span_values,
        side,
    )
    pieces = lax.all_to_all(partial, CTX, split_axis=0, concat_axis=0, tiled=True)
    half = model_dev // 2
    gains = pieces[:, :, width + 2 * GROUP : width + 2 * GROUP + gain_lanes]
    gains = gains.reshape(2 * ctx_size, 1, half).astype(jnp.float32)
    inverse = 1.0 / (gains * gains)
    attended = lax.all_to_all(merge(pieces, ctx_size), CTX, split_axis=0, concat_axis=0, tiled=True)

    tokens = span_total // (2 * ys)
    by_core = attended.reshape(ys, 2, tokens, width)

    def projected(which):
        rows = lax.dynamic_index_in_dim(by_core, which, 1, keepdims=False)
        return jnp.dot(
            rows.reshape(ys * tokens, width), out_weight, preferred_element_type=jnp.float32
        )

    arrived = shifted(projected(1 - core).astype(jnp.bfloat16), "tp_1", 1)
    both = projected(core) + arrived.astype(jnp.float32)
    both = both.reshape(ys, tokens, model_dev)
    stream = residual.astype(jnp.float32) + lax.dynamic_index_in_dim(both, y, 0, keepdims=False)
    sent = both.astype(jnp.bfloat16)
    for by in range(1, ys):
        block = lax.dynamic_index_in_dim(sent, (y + by) % ys, 0, keepdims=False)
        stream = stream + shifted(block, "tp_0", by).astype(jnp.float32)
    gained = (stream * norm_gain.astype(jnp.float32)[None, :]).astype(jnp.bfloat16)
    rows = [gained] + [shifted(gained, "tp_0", by) for by in range(1, ys)]
    rows = jnp.concatenate(rows, 0)

    def places(steps, part):
        dx = jnp.array([s[0] for s in steps], jnp.int32)
        dz = jnp.array([s[1] for s in steps], jnp.int32)
        return 2 * (((x + dx) % xs) * zs + (z + dz) % zs) + part

    def gathered(value, first, second):
        behind, ahead = shifted(value, first, 1), shifted(value, first, -1)
        across = shifted(behind, first, 1)
        near = jnp.stack([value, behind, ahead, across])
        return near, (shifted(near, second, 1), shifted(near, second, -1))

    order = (0, -1, 1, -2)
    near_a, next_a = gathered(rows[:, :half], "ctx_1", "ctx_0")
    near_b, next_b = gathered(rows[:, half:], "ctx_0", "ctx_1")
    at_a = lambda step, among: places([(step, o) for o in among], 0)
    at_b = lambda step, among: places([(o, step) for o in among], 1)
    vocab_dev = head_weight.shape[1]
    mine = lax.dynamic_index_in_dim(targets.reshape(ys, 2, tokens), core, 1, keepdims=False)
    turn = (y - jnp.arange(ys, dtype=jnp.int32)) % ys
    turned = turn[:, None] == jnp.arange(ys, dtype=jnp.int32)[None, :]
    mine = jnp.sum(jnp.where(turned[:, :, None], mine[None], 0), axis=1).reshape(1, -1)
    rank = lax.axis_index(CTX_TP)
    starts = jnp.stack([rank, rank + 1 - 2 * core]) * vocab_dev
    local_target = mine - starts[:, None]
    state = score(
        (near_a, near_b),
        jnp.stack([at_a(0, order), at_b(0, order)]),
        inverse,
        own_weight,
        partner_weight,
        None,
        None,
    )
    next_a, next_b, state = lax.optimization_barrier((next_a, next_b, state))
    far_a, far_b = shifted(next_a[0], "ctx_0", 1), shifted(next_b[0], "ctx_1", 1)
    state = score(
        (*next_a, *next_b),
        jnp.stack([at_a(-1, order), at_a(1, order), at_b(-1, order), at_b(1, order)]),
        inverse,
        own_weight,
        partner_weight,
        state,
        None,
    )
    level_hit = score(
        (far_a, far_b),
        jnp.stack([at_a(-2, order), at_b(-2, order)]),
        inverse,
        own_weight,
        partner_weight,
        state,
        local_target,
    )
    level_hit = level_hit.reshape(2, ys, 1, tokens)
    level_hit = jnp.sum(jnp.where(turned.T[None, :, :, None], level_hit.reshape(2, 1, ys, tokens), 0.0), axis=2)
    gathered_stats = sent_to_all(level_hit.reshape(2, ys * tokens), ("ctx_0", "ctx_1", "tp_0"))
    level, hit = gathered_stats[:, 0], gathered_stats[:, 1]
    top = jnp.max(level, axis=0)
    total = top + jnp.log(jnp.sum(jnp.exp(level - top[None]), axis=0))
    my_logprob = jnp.sum(hit, axis=0) - total
    other_logprob = shifted(my_logprob, "tp_1", 1)
    pair = jnp.stack([my_logprob.reshape(ys, tokens), other_logprob.reshape(ys, tokens)], 1)
    token_logprob = jnp.where(core == 0, pair, pair[:, ::-1]).reshape(span_total)
    window_ends = jnp.cumsum(window_lengths)
    window_starts = window_ends - window_lengths
    positions = jnp.arange(span_total, dtype=jnp.int32)
    member = (positions[None, :] >= window_starts[:, None]) & (
        positions[None, :] < window_ends[:, None]
    )
    window_sums = jnp.sum(jnp.where(member, token_logprob[None, :], 0.0), axis=1)
    window_means = window_sums / window_lengths.astype(jnp.float32)
    own_logprob = lax.dynamic_slice_in_dim(token_logprob, first_token, span_dev, 0)
    return (own_logprob, window_means)


def solution(mesh):
    split = Mesh(mesh.devices.reshape(4, 4, 4, 2), ("ctx_0", "ctx_1", "tp_0", "tp_1"))
    in_specs = (
        P(CTX, TP),
        P(CTX, TP),
        P(CTX, TP),
        P(CTX, TP),
        P(CTX, TP),
        P(TP, CTX),
        P(TP, CTX),
        P(CTX),
        P(None, CTX_TP),
        P(),
        P(),
    )
    out_specs = (P(CTX), P())
    return jax.shard_map(local, mesh=split, in_specs=in_specs, out_specs=out_specs, check_vma=False)
```

```python
import jax
import jax.numpy as jnp
from jax import lax
from jax.experimental import pallas as pl
from jax.experimental.pallas import tpu as pltpu
from jax.sharding import Mesh
from jax.sharding import PartitionSpec as P

D = 8192
HEADS = 64
KV_HEADS = 8
HD = 128
GROUP = HEADS // KV_HEADS
CTX = ("ctx_0", "ctx_1")
TP = ("tp_0", "tp_1")
CTX_TP = ("ctx_0", "ctx_1", "tp_0", "tp_1")
EPSILON = 1e-05
NEGATIVE = -1e30
LOG2E = 1.4426950408889634
TO_LOG2 = HD ** (-0.5) * LOG2E
ROWS = 256
KEYS = 2048
MERGE_ROWS = 16


def sent_to_all(value, axis):
    count = lax.axis_size(axis)
    return lax.all_to_all(
        jnp.broadcast_to(value[None], (count, *value.shape)), axis, 0, 0, tiled=True
    )


def whole(*shape):
    return pl.BlockSpec(shape, lambda *at: (0,) * len(shape))


def copies_of(value, count):
    def body(in_ref, out_ref, sems):
        moves = [
            pltpu.make_async_copy(in_ref, out_ref.at[k], sems.at[k]) for k in range(count)
        ]
        for move in moves:
            move.start()
        for move in moves:
            move.wait()

    return pl.pallas_call(
        body,
        out_shape=jax.ShapeDtypeStruct((count, *value.shape), value.dtype),
        in_specs=[whole(*value.shape)],
        out_specs=pl.BlockSpec(memory_space=pl.ANY),
        grid=(1,),
        scratch_shapes=[pltpu.SemaphoreType.DMA((count,))],
        compiler_params=pltpu.CompilerParams(vmem_limit_bytes=2 << 20),
        name="spread",
    )(value)


def attend(first_token, queries, keys, values, fresh_keys, fresh_values, side):
    sources, span_dev, width = queries.shape
    span, cached, fresh = sources * span_dev, keys.shape[0], fresh_keys.shape[0]
    heads = width // HD
    total = cached + 128
    chunks = [(a, KEYS) for a in range(0, cached, KEYS)]
    chunks[-1] = (chunks[-1][0], total - chunks[-1][0])

    def body(
        first_ref, q_ref, k_ref, v_ref, fk_ref, fv_ref, side_ref, out_ref, kt, va, sbuf, mbuf, sem
    ):
        i = pl.program_id(0)
        load = pltpu.make_async_copy(v_ref, va.at[:cached, :HD], sem)

        @pl.when(i == 0)
        def _():
            load.start()
            for a in range(0, cached, 512):
                kt[:, a : a + 512] = k_ref[a : a + 512, :].T
            gap = jnp.zeros((128 - fresh, HD), jnp.bfloat16)
            kt[:, cached:] = jnp.concatenate([fk_ref[...], gap], 0).T
            va[cached:, :HD] = jnp.concatenate([fv_ref[...], gap], 0)
            va[:, HD:] = jnp.ones((total, HD), jnp.bfloat16)
            out_ref[:, :, width:] = jnp.broadcast_to(side_ref[...], (sources, span_dev, HD))

        def step(scoring, weighing):
            to = lax.rem(i, 2)
            at = lax.rem(i + 1, 2)
            for r in range(0, span, ROWS):
                rows = slice(r, r + ROWS)
                tokens = slice(r // span_dev, (r + ROWS) // span_dev)
                top, acc = None, None
                if scoring:
                    q = q_ref[tokens].reshape(ROWS, HD)
                if weighing:
                    shift = mbuf[at, rows, :]
                for a, n in chunks:
                    if scoring:
                        s = jnp.dot(q, kt[:, a : a + n], preferred_element_type=jnp.float32)
                        if a + n == total:
                            col = lax.broadcasted_iota(jnp.int32, (ROWS, 128), 1)
                            row = lax.broadcasted_iota(jnp.int32, (ROWS, 128), 0) + r
                            seen = (col < fresh) & (row >= col + first_ref[0])
                            tail = jnp.where(seen, s[:, n - 128 :], NEGATIVE)
                            s = jnp.concatenate([s[:, : n - 128], tail], 1)
                        sbuf[to, rows, a : a + n] = s
                        for b in range(0, n, 128):
                            piece = s[:, b : b + 128]
                            top = piece if top is None else jnp.maximum(top, piece)
                    if weighing:
                        p = jnp.concatenate(
                            [
                                jnp.exp2(
                                    sbuf[at, rows, a + b : a + b + 128] * TO_LOG2 - shift
                                ).astype(jnp.bfloat16)
                                for b in range(0, n, 128)
                            ],
                            1,
                        )
                        d = jnp.dot(p, va[a : a + n, :], preferred_element_type=jnp.float32)
                        acc = d if acc is None else acc + d
                if scoring:
                    m = jnp.max(top, axis=1, keepdims=True) * TO_LOG2
                    mbuf[to, rows, :] = jnp.broadcast_to(m, (ROWS, 128))
                if weighing:
                    h = i - 1
                    row_sum = acc[:, HD:]
                    o = (acc[:, :HD] / row_sum).astype(jnp.bfloat16)
                    place = pl.ds(pl.multiple_of(h * HD, HD), HD)
                    out_ref[tokens, :, place] = o.reshape(-1, span_dev, HD)
                    level = shift + jnp.log2(row_sum)
                    high = level.astype(jnp.bfloat16).astype(jnp.float32)
                    low = level - high
                    lane = lax.broadcasted_iota(jnp.int32, (ROWS, HD), 1)
                    old = out_ref[tokens, :, width:].reshape(ROWS, HD).astype(jnp.float32)
                    new = jnp.where(lane == h, high, jnp.where(lane == h + heads, low, old))
                    out_ref[tokens, :, width:] = new.astype(jnp.bfloat16).reshape(-1, span_dev, HD)

        @pl.when(i == 0)
        def _():
            step(True, False)
            load.wait()

        @pl.when((i > 0) & (i < heads))
        def _():
            step(True, True)

        @pl.when(i == heads)
        def _():
            step(False, True)

    out_shape = (sources, span_dev, width + HD)
    return pl.pallas_call(
        body,
        out_shape=jax.ShapeDtypeStruct(out_shape, jnp.bfloat16),
        grid_spec=pltpu.PrefetchScalarGridSpec(
            num_scalar_prefetch=1,
            grid=(heads + 1,),
            in_specs=[
                pl.BlockSpec(
                    (sources, span_dev, HD), lambda i, f: (0, 0, jnp.minimum(i, heads - 1))
                ),
                whole(cached, HD),
                pl.BlockSpec(memory_space=pl.ANY),
                whole(fresh, HD),
                whole(fresh, HD),
                whole(1, span_dev, HD),
            ],
            out_specs=whole(*out_shape),
            scratch_shapes=[
                pltpu.VMEM((HD, total), jnp.bfloat16),
                pltpu.VMEM((total, 2 * HD), jnp.bfloat16),
                pltpu.VMEM((2, span, total), jnp.float32),
                pltpu.VMEM((2, span, HD), jnp.float32),
                pltpu.SemaphoreType.DMA(()),
            ],
        ),
        compiler_params=pltpu.CompilerParams(
            dimension_semantics=("arbitrary",), vmem_limit_bytes=30 << 20
        ),
        cost_estimate=pl.CostEstimate(
            flops=4 * heads * span * total * HD,
            transcendentals=heads * span * total,
            bytes_accessed=6 << 20,
        ),
        name="attend",
    )(first_token, queries, keys, values, fresh_keys, fresh_values, side)


def merge(pieces, copies, before):
    sources, span_dev, wide = pieces.shape
    width = wide - HD
    heads = width // HD
    rows = MERGE_ROWS
    offset = 0 if before is None else before.shape[2]

    def body(in_ref, *refs):
        out_ref = refs[-1]
        tail = in_ref[:, :, width:].astype(jnp.float32).reshape(sources * rows, HD)
        level = (tail + pltpu.roll(tail, HD - heads, 1)).reshape(sources, rows, HD)
        top = jnp.max(level, axis=0)
        weight = jnp.exp2(level - top[None])
        weight = weight / jnp.sum(weight, axis=0)[None]
        if before is not None:
            for k in range(copies):
                out_ref[k, :, :offset] = refs[0][0]
        for h in range(heads):
            cols = slice(h * HD, (h + 1) * HD)
            to = slice(offset + h * HD, offset + (h + 1) * HD)
            acc = None
            for k in range(sources):
                part = in_ref[k, :, cols].astype(jnp.float32) * weight[k][:, h : h + 1]
                acc = part if acc is None else acc + part
            acc = acc.astype(jnp.bfloat16)
            for k in range(copies):
                out_ref[k, :, to] = acc

    operands = [pieces]
    in_specs = [pl.BlockSpec((sources, rows, wide), lambda i: (0, i, 0))]
    if before is not None:
        operands.append(before)
        in_specs.append(pl.BlockSpec((1, rows, offset), lambda i: (0, i, 0)))
    return pl.pallas_call(
        body,
        out_shape=jax.ShapeDtypeStruct((copies, span_dev, offset + width), jnp.bfloat16),
        in_specs=in_specs,
        out_specs=pl.BlockSpec((copies, rows, offset + width), lambda i: (0, i, 0)),
        grid=(span_dev // rows,),
        compiler_params=pltpu.CompilerParams(vmem_limit_bytes=10 << 20),
        cost_estimate=pl.CostEstimate(
            flops=2 * 10**9, transcendentals=0, bytes_accessed=4 * pieces.size
        ),
        name="merge",
    )(*operands)


def score(chunks, places, inverse, own, partner, state, local_target):
    blocks, span, cols = chunks[0].shape
    count = len(chunks)
    vocab = own.shape[0]
    first, last = state is None, local_target is not None
    across = (((1,), (1,)), ((), ()))

    def body(*refs):
        at_ref, *refs = refs
        take = lambda n: [refs.pop(0) for _ in range(n)]
        x_refs, inv_ref = take(count), take(1)[0]
        own_refs, partner_refs = take(count), take(count)
        old = [] if first else take(2)
        t_ref = take(1)[0] if last else None
        acc, squares = (refs[1], refs[2]) if last else (refs[0], refs[1])
        i = pl.program_id(0)

        @pl.when(i == 0)
        def _():
            acc[...] = jnp.zeros_like(acc) if first else old[0][...]
            squares[...] = jnp.zeros_like(squares) if first else old[1][...]

        ss = None
        parts = [x_ref[i] for x_ref in x_refs]
        joint = jnp.concatenate(parts, 1)
        for side, w_refs in enumerate((own_refs, partner_refs)):
            w = jnp.concatenate([w_ref[...] for w_ref in w_refs], 1)
            acc[side] += lax.dot_general(w, joint, across, preferred_element_type=jnp.float32)
        for n, part in enumerate(parts):
            xf = part.astype(jnp.float32)
            sq = xf * xf * inv_ref[at_ref[n, i]]
            for b in range(0, cols, 128):
                piece = sq[:, b : b + 128]
                ss = piece if ss is None else ss + piece
        squares[...] += ss

        if last:

            @pl.when(i == blocks - 1)
            def _():
                mean = jnp.sum(squares[...].T, axis=0, keepdims=True) / D
                scale = lax.rsqrt(mean + EPSILON)
                row = lax.broadcasted_iota(jnp.int32, (vocab, span), 0)
                logits = [acc[side] * scale for side in range(2)]
                top = jnp.max(jnp.maximum(*logits), axis=0, keepdims=True)
                sums = sum(
                    jnp.sum(jnp.exp(part - top), axis=0, keepdims=True) for part in logits
                )
                hit = sum(
                    jnp.sum(
                        jnp.where(row == t_ref[side : side + 1, :], logits[side], 0.0),
                        axis=0,
                        keepdims=True,
                    )
                    for side in range(2)
                )
                refs[0][...] = jnp.concatenate([top + jnp.log(sums), hit], 0)

    kept = [(2, vocab, span), (span, 128)]
    kept_shape = tuple(jax.ShapeDtypeStruct(k, jnp.float32) for k in kept)
    weigh = lambda n: pl.BlockSpec((vocab, cols), lambda i, at: (0, at[n, i]))
    in_specs = [whole(*chunk.shape) for chunk in chunks] + [whole(*inverse.shape)]
    in_specs += [weigh(n) for n in range(count)] * 2
    operands = [*chunks, inverse, *[own] * count, *[partner] * count]
    if not first:
        in_specs += [whole(*k) for k in kept]
        operands += state
    if last:
        in_specs.append(whole(2, span))
        operands.append(local_target)
        out_shape, out_specs = jax.ShapeDtypeStruct((2, span), jnp.float32), whole(2, span)
        scratch = [pltpu.VMEM(k, jnp.float32) for k in kept]
    else:
        out_shape, out_specs, scratch = kept_shape, tuple(whole(*k) for k in kept), []
    return pl.pallas_call(
        body,
        out_shape=out_shape,
        grid_spec=pltpu.PrefetchScalarGridSpec(
            num_scalar_prefetch=1,
            grid=(blocks,),
            in_specs=in_specs,
            out_specs=out_specs,
            scratch_shapes=scratch,
        ),
        compiler_params=pltpu.CompilerParams(
            dimension_semantics=("arbitrary",), vmem_limit_bytes=40 << 20
        ),
        cost_estimate=pl.CostEstimate(
            flops=4 * span * blocks * count * cols * vocab,
            transcendentals=2 * span * vocab if last else 0,
            bytes_accessed=4 * blocks * count * cols * vocab,
        ),
        name="score",
    )(places, *operands)


def shifted(value, axis, by):
    count = lax.axis_size(axis)
    return lax.ppermute(value, axis, [(i, (i + by) % count) for i in range(count)])


def local(
    queries,
    cache_keys,
    cache_values,
    span_keys,
    span_values,
    out_weight,
    residual,
    norm_gain,
    head_weight,
    targets,
    window_lengths,
):
    x, z = lax.axis_index("ctx_0"), lax.axis_index("ctx_1")
    y, core = lax.axis_index("tp_0"), lax.axis_index("tp_1")
    xs, zs, ys = (lax.axis_size(name) for name in ("ctx_0", "ctx_1", "tp_0"))
    ctx_rank = lax.axis_index(CTX)
    span_dev, width = queries.shape
    ctx_size = lax.axis_size(CTX)
    span_total = span_dev * ctx_size
    first_token = ctx_rank * span_dev
    model_dev = norm_gain.shape[0]
    own_weight = head_weight.T
    partner_weight = shifted(own_weight, "tp_1", 1)
    gain_lanes = model_dev // span_dev
    side = jnp.pad(
        norm_gain.reshape(1, span_dev, gain_lanes),
        ((0, 0), (0, 0), (2 * GROUP, HD - 2 * GROUP - gain_lanes)),
    )
    cut = width // 2
    exchanged = lambda value: lax.all_to_all(value, CTX, split_axis=0, concat_axis=0, tiled=True)
    attention = lambda gathered: attend(
        first_token.reshape(1), gathered, cache_keys, cache_values, span_keys, span_values, side
    )
    early, late = copies_of(queries[:, :cut], ctx_size), copies_of(queries[:, cut:], ctx_size)
    early = exchanged(early)
    early, late = lax.optimization_barrier((early, late))
    late = exchanged(late)
    early = attention(early)
    early, late = lax.optimization_barrier((early, late))
    early, late = exchanged(early), attention(late)
    early, late = lax.optimization_barrier((early, late))
    pieces, late = early, exchanged(late)
    half = model_dev // 2
    gains = pieces[:, :, cut + 2 * GROUP : cut + 2 * GROUP + gain_lanes]
    gains = gains.reshape(2 * ctx_size, 1, half).astype(jnp.float32)
    inverse = 1.0 / (gains * gains)
    attended = exchanged(merge(late, ctx_size, merge(pieces, 1, None)))

    tokens = span_total // (2 * ys)
    by_core = attended.reshape(ys, 2, tokens, width)

    def projected(which):
        rows = lax.dynamic_index_in_dim(by_core, which, 1, keepdims=False)
        return jnp.dot(
            rows.reshape(ys * tokens, width), out_weight, preferred_element_type=jnp.float32
        )

    arrived = shifted(projected(1 - core).astype(jnp.bfloat16), "tp_1", 1)
    both = projected(core) + arrived.astype(jnp.float32)
    both = both.reshape(ys, tokens, model_dev)
    stream = residual.astype(jnp.float32) + lax.dynamic_index_in_dim(both, y, 0, keepdims=False)
    sent = both.astype(jnp.bfloat16)
    for by in range(1, ys):
        block = lax.dynamic_index_in_dim(sent, (y + by) % ys, 0, keepdims=False)
        stream = stream + shifted(block, "tp_0", by).astype(jnp.float32)
    gained = (stream * norm_gain.astype(jnp.float32)[None, :]).astype(jnp.bfloat16)
    rows = [gained] + [shifted(gained, "tp_0", by) for by in range(1, ys)]
    rows = jnp.concatenate(rows, 0)

    def places(steps, part):
        dx = jnp.array([s[0] for s in steps], jnp.int32)
        dz = jnp.array([s[1] for s in steps], jnp.int32)
        return 2 * (((x + dx) % xs) * zs + (z + dz) % zs) + part

    def gathered(value, first, second):
        behind, ahead = shifted(value, first, 1), shifted(value, first, -1)
        across = shifted(behind, first, 1)
        near = jnp.stack([value, behind, ahead, across])
        return near, (shifted(near, second, 1), shifted(near, second, -1))

    order = (0, -1, 1, -2)
    near_a, next_a = gathered(rows[:, :half], "ctx_1", "ctx_0")
    near_b, next_b = gathered(rows[:, half:], "ctx_0", "ctx_1")
    at_a = lambda step, among: places([(step, o) for o in among], 0)
    at_b = lambda step, among: places([(o, step) for o in among], 1)
    vocab_dev = head_weight.shape[1]
    mine = lax.dynamic_index_in_dim(targets.reshape(ys, 2, tokens), core, 1, keepdims=False)
    turn = (y - jnp.arange(ys, dtype=jnp.int32)) % ys
    turned = turn[:, None] == jnp.arange(ys, dtype=jnp.int32)[None, :]
    mine = jnp.sum(jnp.where(turned[:, :, None], mine[None], 0), axis=1).reshape(1, -1)
    rank = lax.axis_index(CTX_TP)
    starts = jnp.stack([rank, rank + 1 - 2 * core]) * vocab_dev
    local_target = mine - starts[:, None]
    state = score(
        (near_a, near_b),
        jnp.stack([at_a(0, order), at_b(0, order)]),
        inverse,
        own_weight,
        partner_weight,
        None,
        None,
    )
    next_a, next_b, state = lax.optimization_barrier((next_a, next_b, state))
    far_a, far_b = shifted(next_a[0], "ctx_0", 1), shifted(next_b[0], "ctx_1", 1)
    state = score(
        (*next_a, *next_b),
        jnp.stack([at_a(-1, order), at_a(1, order), at_b(-1, order), at_b(1, order)]),
        inverse,
        own_weight,
        partner_weight,
        state,
        None,
    )
    level_hit = score(
        (far_a, far_b),
        jnp.stack([at_a(-2, order), at_b(-2, order)]),
        inverse,
        own_weight,
        partner_weight,
        state,
        local_target,
    )
    level_hit = level_hit.reshape(2, ys, 1, tokens)
    level_hit = jnp.sum(jnp.where(turned.T[None, :, :, None], level_hit.reshape(2, 1, ys, tokens), 0.0), axis=2)
    gathered_stats = sent_to_all(level_hit.reshape(2, ys * tokens), ("ctx_0", "ctx_1", "tp_0"))
    level, hit = gathered_stats[:, 0], gathered_stats[:, 1]
    top = jnp.max(level, axis=0)
    total = top + jnp.log(jnp.sum(jnp.exp(level - top[None]), axis=0))
    my_logprob = jnp.sum(hit, axis=0) - total
    other_logprob = shifted(my_logprob, "tp_1", 1)
    pair = jnp.stack([my_logprob.reshape(ys, tokens), other_logprob.reshape(ys, tokens)], 1)
    token_logprob = jnp.where(core == 0, pair, pair[:, ::-1]).reshape(span_total)
    window_ends = jnp.cumsum(window_lengths)
    window_starts = window_ends - window_lengths
    positions = jnp.arange(span_total, dtype=jnp.int32)
    member = (positions[None, :] >= window_starts[:, None]) & (
        positions[None, :] < window_ends[:, None]
    )
    window_sums = jnp.sum(jnp.where(member, token_logprob[None, :], 0.0), axis=1)
    window_means = window_sums / window_lengths.astype(jnp.float32)
    own_logprob = lax.dynamic_slice_in_dim(token_logprob, first_token, span_dev, 0)
    return (own_logprob, window_means)


def solution(mesh):
    split = Mesh(mesh.devices.reshape(4, 4, 4, 2), ("ctx_0", "ctx_1", "tp_0", "tp_1"))
    in_specs = (
        P(CTX, TP),
        P(CTX, TP),
        P(CTX, TP),
        P(CTX, TP),
        P(CTX, TP),
        P(TP, CTX),
        P(TP, CTX),
        P(CTX),
        P(None, CTX_TP),
        P(),
        P(),
    )
    out_specs = (P(CTX), P())
    return jax.shard_map(local, mesh=split, in_specs=in_specs, out_specs=out_specs, check_vma=False)
```

```python
import jax
import jax.numpy as jnp
from jax import lax
from jax.experimental import pallas as pl
from jax.experimental.pallas import tpu as pltpu
from jax.sharding import Mesh
from jax.sharding import PartitionSpec as P

D = 8192
HEADS = 64
KV_HEADS = 8
HD = 128
GROUP = HEADS // KV_HEADS
CTX = ("ctx_0", "ctx_1")
TP = ("tp_0", "tp_1")
CTX_TP = ("ctx_0", "ctx_1", "tp_0", "tp_1")
EPSILON = 1e-05
NEGATIVE = -1e30
LOG2E = 1.4426950408889634
TO_LOG2 = HD ** (-0.5) * LOG2E
ROWS = 256
KEYS = 2048
MERGE_ROWS = 16


def sent_to_all(value, axis):
    count = lax.axis_size(axis)
    return lax.all_to_all(
        jnp.broadcast_to(value[None], (count, *value.shape)), axis, 0, 0, tiled=True
    )


def whole(*shape):
    return pl.BlockSpec(shape, lambda *at: (0,) * len(shape))


def copies_of(value, count):
    def body(in_ref, out_ref, sems):
        moves = [
            pltpu.make_async_copy(in_ref, out_ref.at[k], sems.at[k]) for k in range(count)
        ]
        for move in moves:
            move.start()
        for move in moves:
            move.wait()

    return pl.pallas_call(
        body,
        out_shape=jax.ShapeDtypeStruct((count, *value.shape), value.dtype),
        in_specs=[whole(*value.shape)],
        out_specs=pl.BlockSpec(memory_space=pl.ANY),
        grid=(1,),
        scratch_shapes=[pltpu.SemaphoreType.DMA((count,))],
        compiler_params=pltpu.CompilerParams(vmem_limit_bytes=2 << 20),
        name="spread",
    )(value)


def attend(first_token, queries, keys, values, fresh_keys, fresh_values, side):
    sources, span_dev, width = queries.shape
    span, cached, fresh = sources * span_dev, keys.shape[0], fresh_keys.shape[0]
    heads = width // HD
    total = cached + 128
    chunks = [(a, KEYS) for a in range(0, cached, KEYS)]
    chunks[-1] = (chunks[-1][0], total - chunks[-1][0])

    def body(
        first_ref, q_ref, k_ref, v_ref, fk_ref, fv_ref, side_ref, out_ref, kt, va, sbuf, mbuf, sem
    ):
        i = pl.program_id(0)
        load = pltpu.make_async_copy(v_ref, va.at[:cached, :HD], sem)

        @pl.when(i == 0)
        def _():
            load.start()
            for a in range(0, cached, 512):
                kt[:, a : a + 512] = k_ref[a : a + 512, :].T
            gap = jnp.zeros((128 - fresh, HD), jnp.bfloat16)
            kt[:, cached:] = jnp.concatenate([fk_ref[...], gap], 0).T
            va[cached:, :HD] = jnp.concatenate([fv_ref[...], gap], 0)
            va[:, HD:] = jnp.ones((total, HD), jnp.bfloat16)
            out_ref[:, :, width:] = jnp.broadcast_to(side_ref[...], (sources, span_dev, HD))

        def step(scoring, weighing):
            to = lax.rem(i, 2)
            at = lax.rem(i + 1, 2)
            for r in range(0, span, ROWS):
                rows = slice(r, r + ROWS)
                tokens = slice(r // span_dev, (r + ROWS) // span_dev)
                top, acc = None, None
                if scoring:
                    q = q_ref[tokens].reshape(ROWS, HD)
                if weighing:
                    shift = mbuf[at, rows, :]
                for a, n in chunks:
                    if scoring:
                        s = jnp.dot(q, kt[:, a : a + n], preferred_element_type=jnp.float32)
                        if a + n == total:
                            col = lax.broadcasted_iota(jnp.int32, (ROWS, 128), 1)
                            row = lax.broadcasted_iota(jnp.int32, (ROWS, 128), 0) + r
                            seen = (col < fresh) & (row >= col + first_ref[0])
                            tail = jnp.where(seen, s[:, n - 128 :], NEGATIVE)
                            s = jnp.concatenate([s[:, : n - 128], tail], 1)
                        sbuf[to, rows, a : a + n] = s
                        for b in range(0, n, 128):
                            piece = s[:, b : b + 128]
                            top = piece if top is None else jnp.maximum(top, piece)
                    if weighing:
                        p = jnp.concatenate(
                            [
                                jnp.exp2(
                                    sbuf[at, rows, a + b : a + b + 128] * TO_LOG2 - shift
                                ).astype(jnp.bfloat16)
                                for b in range(0, n, 128)
                            ],
                            1,
                        )
                        d = jnp.dot(p, va[a : a + n, :], preferred_element_type=jnp.float32)
                        acc = d if acc is None else acc + d
                if scoring:
                    m = jnp.max(top, axis=1, keepdims=True) * TO_LOG2
                    mbuf[to, rows, :] = jnp.broadcast_to(m, (ROWS, 128))
                if weighing:
                    h = i - 1
                    row_sum = acc[:, HD:]
                    o = (acc[:, :HD] / row_sum).astype(jnp.bfloat16)
                    place = pl.ds(pl.multiple_of(h * HD, HD), HD)
                    out_ref[tokens, :, place] = o.reshape(-1, span_dev, HD)
                    level = shift + jnp.log2(row_sum)
                    high = level.astype(jnp.bfloat16).astype(jnp.float32)
                    low = level - high
                    lane = lax.broadcasted_iota(jnp.int32, (ROWS, HD), 1)
                    old = out_ref[tokens, :, width:].reshape(ROWS, HD).astype(jnp.float32)
                    new = jnp.where(lane == h, high, jnp.where(lane == h + heads, low, old))
                    out_ref[tokens, :, width:] = new.astype(jnp.bfloat16).reshape(-1, span_dev, HD)

        @pl.when(i == 0)
        def _():
            step(True, False)
            load.wait()

        @pl.when((i > 0) & (i < heads))
        def _():
            step(True, True)

        @pl.when(i == heads)
        def _():
            step(False, True)

    out_shape = (sources, span_dev, width + HD)
    return pl.pallas_call(
        body,
        out_shape=jax.ShapeDtypeStruct(out_shape, jnp.bfloat16),
        grid_spec=pltpu.PrefetchScalarGridSpec(
            num_scalar_prefetch=1,
            grid=(heads + 1,),
            in_specs=[
                pl.BlockSpec(
                    (sources, span_dev, HD), lambda i, f: (0, 0, jnp.minimum(i, heads - 1))
                ),
                whole(cached, HD),
                pl.BlockSpec(memory_space=pl.ANY),
                whole(fresh, HD),
                whole(fresh, HD),
                whole(1, span_dev, HD),
            ],
            out_specs=whole(*out_shape),
            scratch_shapes=[
                pltpu.VMEM((HD, total), jnp.bfloat16),
                pltpu.VMEM((total, 2 * HD), jnp.bfloat16),
                pltpu.VMEM((2, span, total), jnp.float32),
                pltpu.VMEM((2, span, HD), jnp.float32),
                pltpu.SemaphoreType.DMA(()),
            ],
        ),
        compiler_params=pltpu.CompilerParams(
            dimension_semantics=("arbitrary",), vmem_limit_bytes=30 << 20
        ),
        cost_estimate=pl.CostEstimate(
            flops=4 * heads * span * total * HD,
            transcendentals=heads * span * total,
            bytes_accessed=6 << 20,
        ),
        name="attend",
    )(first_token, queries, keys, values, fresh_keys, fresh_values, side)


def merge(pieces, copies):
    sources, span_dev, wide = pieces.shape
    width = wide - HD
    heads = width // HD
    rows = MERGE_ROWS

    def body(in_ref, out_ref):
        tail = in_ref[:, :, width:].astype(jnp.float32).reshape(sources * rows, HD)
        level = (tail + pltpu.roll(tail, HD - heads, 1)).reshape(sources, rows, HD)
        top = jnp.max(level, axis=0)
        weight = jnp.exp2(level - top[None])
        weight = weight / jnp.sum(weight, axis=0)[None]
        for h in range(heads):
            cols = slice(h * HD, (h + 1) * HD)
            acc = None
            for k in range(sources):
                part = in_ref[k, :, cols].astype(jnp.float32) * weight[k][:, h : h + 1]
                acc = part if acc is None else acc + part
            acc = acc.astype(jnp.bfloat16)
            for k in range(copies):
                out_ref[k, :, cols] = acc

    return pl.pallas_call(
        body,
        out_shape=jax.ShapeDtypeStruct((copies, span_dev, width), jnp.bfloat16),
        in_specs=[pl.BlockSpec((sources, rows, wide), lambda i: (0, i, 0))],
        out_specs=pl.BlockSpec((copies, rows, width), lambda i: (0, i, 0)),
        grid=(span_dev // rows,),
        compiler_params=pltpu.CompilerParams(vmem_limit_bytes=10 << 20),
        name="merge",
    )(pieces)


def arranged(places, weight, cols):
    vocab = weight.shape[0]
    count = places.shape[0]

    def body(at_ref, w_ref, out_ref, buf, read, written):
        def load(j):
            place = pl.ds(pl.multiple_of(at_ref[j] * cols, cols), cols)
            return pltpu.make_async_copy(w_ref.at[:, place], buf.at[j], read.at[j])

        def store(j):
            return pltpu.make_async_copy(buf.at[j], out_ref.at[j], written.at[j])

        for j in range(count):
            load(j).start()
        for j in range(count):
            load(j).wait()
            store(j).start()
        for j in range(count):
            store(j).wait()

    return pl.pallas_call(
        body,
        out_shape=jax.ShapeDtypeStruct((count, vocab, cols), weight.dtype),
        grid_spec=pltpu.PrefetchScalarGridSpec(
            num_scalar_prefetch=1,
            grid=(1,),
            in_specs=[pl.BlockSpec(memory_space=pl.ANY)],
            out_specs=pl.BlockSpec(memory_space=pl.ANY),
            scratch_shapes=[
                pltpu.VMEM((count, vocab, cols), weight.dtype),
                pltpu.SemaphoreType.DMA((count,)),
                pltpu.SemaphoreType.DMA((count,)),
            ],
        ),
        compiler_params=pltpu.CompilerParams(
            dimension_semantics=("arbitrary",), vmem_limit_bytes=58 << 20
        ),
        cost_estimate=pl.CostEstimate(
            flops=10**10, transcendentals=0, bytes_accessed=4 * count * vocab * cols
        ),
        name="arrange",
    )(places, weight)


def score(chunks, places, inverse, own, partner, base, state, local_target):
    blocks, span, cols = chunks[0].shape
    count = len(chunks)
    vocab = own.shape[-2]
    first, last = state is None, local_target is not None
    across = (((1,), (1,)), ((), ()))

    def body(*refs):
        at_ref, *refs = refs
        take = lambda n: [refs.pop(0) for _ in range(n)]
        x_refs, inv_ref = take(count), take(1)[0]
        own_refs, partner_refs = take(count), take(count)
        old = [] if first else take(2)
        t_ref = take(1)[0] if last else None
        acc, squares = (refs[1], refs[2]) if last else (refs[0], refs[1])
        i = pl.program_id(0)

        @pl.when(i == 0)
        def _():
            acc[...] = jnp.zeros_like(acc) if first else old[0][...]
            squares[...] = jnp.zeros_like(squares) if first else old[1][...]

        ss = None
        parts = [x_ref[i] for x_ref in x_refs]
        joint = jnp.concatenate(parts, 1)
        for side, w_refs in enumerate((own_refs, partner_refs)):
            w = jnp.concatenate([w_ref[...] for w_ref in w_refs], 1)
            acc[side] += lax.dot_general(w, joint, across, preferred_element_type=jnp.float32)
        for n, part in enumerate(parts):
            xf = part.astype(jnp.float32)
            sq = xf * xf * inv_ref[at_ref[n, i]]
            for b in range(0, cols, 128):
                piece = sq[:, b : b + 128]
                ss = piece if ss is None else ss + piece
        squares[...] += ss

        if last:

            @pl.when(i == blocks - 1)
            def _():
                mean = jnp.sum(squares[...].T, axis=0, keepdims=True) / D
                scale = lax.rsqrt(mean + EPSILON)
                row = lax.broadcasted_iota(jnp.int32, (vocab, span), 0)
                logits = [acc[side] * scale for side in range(2)]
                top = jnp.max(jnp.maximum(*logits), axis=0, keepdims=True)
                sums = sum(
                    jnp.sum(jnp.exp(part - top), axis=0, keepdims=True) for part in logits
                )
                hit = sum(
                    jnp.sum(
                        jnp.where(row == t_ref[side : side + 1, :], logits[side], 0.0),
                        axis=0,
                        keepdims=True,
                    )
                    for side in range(2)
                )
                refs[0][...] = jnp.concatenate([top + jnp.log(sums), hit], 0)

    kept = [(2, vocab, span), (span, 128)]
    kept_shape = tuple(jax.ShapeDtypeStruct(k, jnp.float32) for k in kept)
    if base is None:
        weigh = lambda n: pl.BlockSpec((vocab, cols), lambda i, at: (0, at[n, i]))
    else:
        weigh = lambda n: pl.BlockSpec(
            (None, vocab, cols), lambda i, at: (base + n * blocks + i, 0, 0)
        )
    in_specs = [whole(*chunk.shape) for chunk in chunks] + [whole(*inverse.shape)]
    in_specs += [weigh(n) for n in range(count)] * 2
    operands = [*chunks, inverse, *[own] * count, *[partner] * count]
    if not first:
        in_specs += [whole(*k) for k in kept]
        operands += state
    if last:
        in_specs.append(whole(2, span))
        operands.append(local_target)
        out_shape, out_specs = jax.ShapeDtypeStruct((2, span), jnp.float32), whole(2, span)
        scratch = [pltpu.VMEM(k, jnp.float32) for k in kept]
    else:
        out_shape, out_specs, scratch = kept_shape, tuple(whole(*k) for k in kept), []
    return pl.pallas_call(
        body,
        out_shape=out_shape,
        grid_spec=pltpu.PrefetchScalarGridSpec(
            num_scalar_prefetch=1,
            grid=(blocks,),
            in_specs=in_specs,
            out_specs=out_specs,
            scratch_shapes=scratch,
        ),
        compiler_params=pltpu.CompilerParams(
            dimension_semantics=("arbitrary",), vmem_limit_bytes=40 << 20
        ),
        cost_estimate=pl.CostEstimate(
            flops=4 * span * blocks * count * cols * vocab,
            transcendentals=2 * span * vocab if last else 0,
            bytes_accessed=4 * blocks * count * cols * vocab,
        ),
        name="score",
    )(places, *operands)


def shifted(value, axis, by):
    count = lax.axis_size(axis)
    return lax.ppermute(value, axis, [(i, (i + by) % count) for i in range(count)])


def local(
    queries,
    cache_keys,
    cache_values,
    span_keys,
    span_values,
    out_weight,
    residual,
    norm_gain,
    head_weight,
    targets,
    window_lengths,
):
    x, z = lax.axis_index("ctx_0"), lax.axis_index("ctx_1")
    y, core = lax.axis_index("tp_0"), lax.axis_index("tp_1")
    xs, zs, ys = (lax.axis_size(name) for name in ("ctx_0", "ctx_1", "tp_0"))
    ctx_rank = lax.axis_index(CTX)
    span_dev, width = queries.shape
    ctx_size = lax.axis_size(CTX)
    span_total = span_dev * ctx_size
    first_token = ctx_rank * span_dev
    model_dev = norm_gain.shape[0]
    own_weight = head_weight.T
    partner_weight = shifted(own_weight, "tp_1", 1)
    gain_lanes = model_dev // span_dev
    half = model_dev // 2
    def places(steps, part):
        dx = jnp.array([s[0] for s in steps], jnp.int32)
        dz = jnp.array([s[1] for s in steps], jnp.int32)
        return 2 * (((x + dx) % xs) * zs + (z + dz) % zs) + part

    order = (0, -1, 1, -2)
    at_a = lambda step, among: places([(step, o) for o in among], 0)
    at_b = lambda step, among: places([(o, step) for o in among], 1)
    next_at = jnp.stack([at_a(-1, order), at_a(1, order), at_b(-1, order), at_b(1, order)])
    far_at = jnp.stack([at_a(-2, order), at_b(-2, order)])
    wanted = jnp.concatenate([next_at, far_at]).reshape(-1)
    own_blocks = arranged(wanted, own_weight, half)
    side = jnp.pad(
        norm_gain.reshape(1, span_dev, gain_lanes),
        ((0, 0), (0, 0), (2 * GROUP, HD - 2 * GROUP - gain_lanes)),
    )
    side, own_blocks = lax.optimization_barrier((side, own_blocks))
    partial = attend(
        first_token.reshape(1),
        lax.all_to_all(copies_of(queries, ctx_size), CTX, 0, 0, tiled=True),
        cache_keys,
        cache_values,
        span_keys,
        span_values,
        side,
    )
    pieces = lax.all_to_all(partial, CTX, split_axis=0, concat_axis=0, tiled=True)
    merged = merge(pieces, ctx_size)
    merged, wanted = lax.optimization_barrier((merged, wanted))
    partner_blocks = arranged(wanted, partner_weight, half)
    gains = pieces[:, :, width + 2 * GROUP : width + 2 * GROUP + gain_lanes]
    gains = gains.reshape(2 * ctx_size, 1, half).astype(jnp.float32)
    inverse = 1.0 / (gains * gains)
    attended = lax.all_to_all(merged, CTX, split_axis=0, concat_axis=0, tiled=True)
    attended, partner_blocks = lax.optimization_barrier((attended, partner_blocks))

    tokens = span_total // (2 * ys)
    by_core = attended.reshape(ys, 2, tokens, width)

    def projected(which):
        rows = lax.dynamic_index_in_dim(by_core, which, 1, keepdims=False)
        return jnp.dot(
            rows.reshape(ys * tokens, width), out_weight, preferred_element_type=jnp.float32
        )

    arrived = shifted(projected(1 - core).astype(jnp.bfloat16), "tp_1", 1)
    both = projected(core) + arrived.astype(jnp.float32)
    both = both.reshape(ys, tokens, model_dev)
    stream = residual.astype(jnp.float32) + lax.dynamic_index_in_dim(both, y, 0, keepdims=False)
    sent = both.astype(jnp.bfloat16)
    for by in range(1, ys):
        block = lax.dynamic_index_in_dim(sent, (y + by) % ys, 0, keepdims=False)
        stream = stream + shifted(block, "tp_0", by).astype(jnp.float32)
    gained = (stream * norm_gain.astype(jnp.float32)[None, :]).astype(jnp.bfloat16)
    rows = [gained] + [shifted(gained, "tp_0", by) for by in range(1, ys)]
    rows = jnp.concatenate(rows, 0)

    def gathered(value, first, second):
        behind, ahead = shifted(value, first, 1), shifted(value, first, -1)
        across = shifted(behind, first, 1)
        near = jnp.stack([value, behind, ahead, across])
        return near, (shifted(near, second, 1), shifted(near, second, -1))

    near_a, next_a = gathered(rows[:, :half], "ctx_1", "ctx_0")
    near_b, next_b = gathered(rows[:, half:], "ctx_0", "ctx_1")
    vocab_dev = head_weight.shape[1]
    mine = lax.dynamic_index_in_dim(targets.reshape(ys, 2, tokens), core, 1, keepdims=False)
    turn = (y - jnp.arange(ys, dtype=jnp.int32)) % ys
    turned = turn[:, None] == jnp.arange(ys, dtype=jnp.int32)[None, :]
    mine = jnp.sum(jnp.where(turned[:, :, None], mine[None], 0), axis=1).reshape(1, -1)
    rank = lax.axis_index(CTX_TP)
    starts = jnp.stack([rank, rank + 1 - 2 * core]) * vocab_dev
    local_target = mine - starts[:, None]
    state = score(
        (near_a, near_b),
        jnp.stack([at_a(0, order), at_b(0, order)]),
        inverse,
        own_weight,
        partner_weight,
        None,
        None,
        None,
    )
    next_a, next_b, state = lax.optimization_barrier((next_a, next_b, state))
    far_a, far_b = shifted(next_a[0], "ctx_0", 1), shifted(next_b[0], "ctx_1", 1)
    state = score(
        (*next_a, *next_b),
        next_at,
        inverse,
        own_blocks,
        partner_blocks,
        0,
        state,
        None,
    )
    level_hit = score(
        (far_a, far_b),
        far_at,
        inverse,
        own_blocks,
        partner_blocks,
        next_at.size,
        state,
        local_target,
    )
    level_hit = level_hit.reshape(2, ys, 1, tokens)
    level_hit = jnp.sum(jnp.where(turned.T[None, :, :, None], level_hit.reshape(2, 1, ys, tokens), 0.0), axis=2)
    gathered_stats = sent_to_all(level_hit.reshape(2, ys * tokens), ("ctx_0", "ctx_1", "tp_0"))
    level, hit = gathered_stats[:, 0], gathered_stats[:, 1]
    top = jnp.max(level, axis=0)
    total = top + jnp.log(jnp.sum(jnp.exp(level - top[None]), axis=0))
    my_logprob = jnp.sum(hit, axis=0) - total
    other_logprob = shifted(my_logprob, "tp_1", 1)
    pair = jnp.stack([my_logprob.reshape(ys, tokens), other_logprob.reshape(ys, tokens)], 1)
    token_logprob = jnp.where(core == 0, pair, pair[:, ::-1]).reshape(span_total)
    window_ends = jnp.cumsum(window_lengths)
    window_starts = window_ends - window_lengths
    positions = jnp.arange(span_total, dtype=jnp.int32)
    member = (positions[None, :] >= window_starts[:, None]) & (
        positions[None, :] < window_ends[:, None]
    )
    window_sums = jnp.sum(jnp.where(member, token_logprob[None, :], 0.0), axis=1)
    window_means = window_sums / window_lengths.astype(jnp.float32)
    own_logprob = lax.dynamic_slice_in_dim(token_logprob, first_token, span_dev, 0)
    return (own_logprob, window_means)


def solution(mesh):
    split = Mesh(mesh.devices.reshape(4, 4, 4, 2), ("ctx_0", "ctx_1", "tp_0", "tp_1"))
    in_specs = (
        P(CTX, TP),
        P(CTX, TP),
        P(CTX, TP),
        P(CTX, TP),
        P(CTX, TP),
        P(TP, CTX),
        P(TP, CTX),
        P(CTX),
        P(None, CTX_TP),
        P(),
        P(),
    )
    out_specs = (P(CTX), P())
    return jax.shard_map(local, mesh=split, in_specs=in_specs, out_specs=out_specs, check_vma=False)
```
